128 devices in a mesh: node: 8 (over z, core), local: 16 (over y, x).
Axes of the slice: x: 4, y: 4, z: 4, core: 2. Of those that a mesh axis runs over, the one named last changes fastest.
Arguments:
- tokens: bfloat16 [2048, 7168], P(('node', 'local')), may hold values from -6 to 6
- grad_out: bfloat16 [2048, 7168], P(('node', 'local')), may hold values from -6 to 6
- gates: bfloat16 [2048, 3], P(('node', 'local')), may hold values from 0.19921875 to 1
- expert_ids: int32 [2048, 3], P(('node', 'local')), may hold values from 0 to 15, as said below
- w_gate: bfloat16 [8, 7168, 2048], P('node', None, 'local'), may hold values from -0.0625 to 0.0625
- w_up: bfloat16 [8, 7168, 2048], P('node', None, 'local'), may hold values from -0.0625 to 0.0625
- w_down: bfloat16 [8, 7168, 2048], P('node', None, 'local'), may hold values from -0.1875 to 0.1875
- s_gate: bfloat16 [7168, 2048], P(None, 'local'), may hold values from -0.0625 to 0.0625
- s_up: bfloat16 [7168, 2048], P(None, 'local'), may hold values from -0.0625 to 0.0625
- s_down: bfloat16 [7168, 2048], P(None, 'local'), may hold values from -0.125 to 0.125
Outputs:
- dx: bfloat16 [2048, 7168], P(('node', 'local'))
- dgates: float32 [2048, 3], P(('node', 'local'))
- d_w_gate: bfloat16 [8, 7168, 2048], P('node', None, 'local')
- d_w_up: bfloat16 [8, 7168, 2048], P('node', None, 'local')
- d_w_down: bfloat16 [8, 7168, 2048], P('node', None, 'local')
- d_s_gate: bfloat16 [7168, 2048], P('node', 'local')
- d_s_up: bfloat16 [7168, 2048], P('node', 'local')
- d_s_down: bfloat16 [7168, 2048], P('node', 'local')
The draws below stay inside these ranges and needn't reach their ends.
Inputs may be any that keep to these rules, and one draw needn't show every extreme that they name: `expert_ids`: each token names both experts of one node and one expert of a second node. Of the tokens of one device exactly 4 name experts of each node and at most 4 name any one expert; for every node one of its experts is named by exactly 4 tokens of every device.
All inputs are finite; a program needn't handle non-finite values.
Results may differ from the reference program's by a relative error of at most 0.014.
Values may be sent and summed in bfloat16 or wider, within the bound.
A program may use at most 192 MiB of HBM per device.

```python
import jax
import jax.numpy as jnp
from jax import lax

D = 7168
FF = 1024
FFS = 2048
TOPK = 3
E_NODE = 2
TOK_DEV = 16
TOKENS = 2048
EXPERTS = 16
N_NODE = 8
N_LOCAL = 16


def draw_expert_ids(key, part):
    node_count = EXPERTS // E_NODE
    device_count = TOKENS // TOK_DEV
    keys = jax.random.split(key, 4)
    node_order = jax.vmap(lambda item: jax.random.permutation(item, node_count))(jax.random.split(keys[0], device_count))
    position = jnp.arange(TOK_DEV, dtype=jnp.int32)
    first_slot = position % node_count
    second_slot = (first_slot + 1 + position // node_count % (node_count - 1)) % node_count
    first = jnp.take(node_order, first_slot, axis=1)
    second = jnp.take(node_order, second_slot, axis=1)
    busy = jax.random.randint(keys[1], (node_count,), 0, E_NODE)
    single = jnp.take(busy, second)
    trio = jnp.stack([first * E_NODE, first * E_NODE + 1, second * E_NODE + single], axis=-1)
    shift = jax.random.randint(keys[2], (device_count, TOK_DEV, 1), 0, 3)
    column = (jnp.arange(3, dtype=jnp.int32)[None, None, :] + shift) % 3
    trio = jnp.take_along_axis(trio, column, axis=2)
    shuffle = jax.vmap(lambda item: jax.random.permutation(item, TOK_DEV))(jax.random.split(keys[3], device_count))
    trio = jnp.take_along_axis(trio, shuffle[:, :, None], axis=1)
    return trio.reshape(TOKENS, 3).astype(jnp.int32)


def shard_levels(stream_key, extent, shards, least, top_value):
    loudness, own = 1.0, jax.random.fold_in(stream_key, 6)
    for dim, blocks in shards:
        heights = jnp.exp(jax.random.uniform(jax.random.fold_in(own, dim), (blocks,), jnp.float32, least / len(shards), top_value / len(shards)))
        loudness = loudness * jnp.repeat(heights, extent[dim] // blocks).reshape([-1 if axis == dim else 1 for axis in range(len(extent))])
    return loudness


def bell_draw(own_key, extent, deviation, bound, shards=(), kind=jnp.bfloat16):
    factor_of = shard_levels(own_key, extent, shards, -0.22, 0.18) if shards else 1.0
    array = jax.random.normal(own_key, extent, jnp.float32) * deviation * factor_of
    return jnp.minimum(jnp.maximum(array, -bound), bound).astype(kind)


def setup_inputs(seed: int = 0) -> dict:
    key_of = jax.random.split(jax.random.key(seed), 11)
    tokens = bell_draw(key_of[0], (TOKENS, D), 1.0, 6.0, ((0, 128),))
    grad_out = bell_draw(key_of[1], (TOKENS, D), 1.0, 6.0, ((0, 128),))
    gates = jnp.clip(0.19921875 + 0.80078125 * jax.random.uniform(key_of[2], (TOKENS, TOPK), jnp.float32) ** shard_levels(key_of[2], (TOKENS, TOPK), ((0, 128),), -0.2, 0.2), 0.19921875, 1.0).astype(jnp.bfloat16)
    expert_ids = draw_expert_ids(jax.random.fold_in(key_of[10], 71), 0)
    w_gate = bell_draw(key_of[4], (N_NODE, D, E_NODE * FF), D ** -0.5, 0.0625, ((0, 8), (2, 16)))
    w_up = bell_draw(key_of[5], (N_NODE, D, E_NODE * FF), D ** -0.5, 0.0625, ((0, 8), (2, 16)))
    w_down = bell_draw(key_of[6], (N_NODE, D, E_NODE * FF), FF ** -0.5, 0.1875, ((0, 8), (2, 16)))
    s_gate = bell_draw(key_of[7], (D, FFS), D ** -0.5, 0.0625, ((1, 16),))
    s_up = bell_draw(key_of[8], (D, FFS), D ** -0.5, 0.0625, ((1, 16),))
    s_down = bell_draw(key_of[9], (D, FFS), FFS ** -0.5, 0.125, ((1, 16),))
    return {"tokens": tokens, "grad_out": grad_out, "gates": gates, "expert_ids": expert_ids, "w_gate": w_gate, "w_up": w_up, "w_down": w_down, "s_gate": s_gate, "s_up": s_up, "s_down": s_down}


def silu_parts(pre_gate):
    sig = jax.nn.sigmoid(pre_gate)
    return pre_gate * sig, sig * (1.0 + pre_gate * (1.0 - sig))


def contract_first(left, right):
    return lax.dot_general(left, right, (((0,), (0,)), ((), ())), preferred_element_type=jnp.float32)


def contract_last(left, right):
    return lax.dot_general(left, right, (((1,), (1,)), ((), ())), preferred_element_type=jnp.float32)


def ffn_backward(rows_in, rows_grad, weight, gate_w, up_w, down_w):
    pre_gate = jnp.dot(rows_in, gate_w, preferred_element_type=jnp.float32)
    pre_up = jnp.dot(rows_in, up_w, preferred_element_type=jnp.float32)
    activ, slope = silu_parts(pre_gate)
    hidden = activ * pre_up
    upstream = jnp.dot(rows_grad, down_w, preferred_element_type=jnp.float32)
    scaled = weight * upstream
    grad_up = (scaled * activ).astype(jnp.bfloat16)
    grad_gate = (scaled * pre_up * slope).astype(jnp.bfloat16)
    weighted = (weight * hidden).astype(jnp.bfloat16)
    return grad_gate, grad_up, weighted, hidden * upstream


def block_rows(grad_gate, grad_up, gate_w, up_w, width):
    blocks = gate_w.shape[1] // width

    def step(index, total):
        start = index * width
        part = contract_last(lax.dynamic_slice_in_dim(grad_gate, start, width, 1), lax.dynamic_slice_in_dim(gate_w, start, width, 1))
        part = part + contract_last(lax.dynamic_slice_in_dim(grad_up, start, width, 1), lax.dynamic_slice_in_dim(up_w, start, width, 1))
        rounded = lax.optimization_barrier(part.astype(jnp.bfloat16))
        return total + rounded.astype(jnp.float32)

    return lax.fori_loop(0, blocks, step, jnp.zeros((grad_gate.shape[0], gate_w.shape[0]), jnp.float32))


def block_stat(product, width):
    sums = jnp.sum(product.reshape(product.shape[0], -1, width), axis=2)
    return jnp.sum(lax.optimization_barrier(sums.astype(jnp.bfloat16)).astype(jnp.float32), axis=1)


def reference(tokens, grad_out, gates, expert_ids, w_gate, w_up, w_down, s_gate, s_up, s_down):
    n_tok = tokens.shape[0]
    width = tokens.shape[1]
    device_count = n_tok // TOK_DEV
    slots = device_count * (2 * TOK_DEV // N_NODE)
    group_size = N_LOCAL // E_NODE
    ff_block = FF // group_size
    gate_all = gates.astype(jnp.float32)
    positions = jnp.arange(n_tok, dtype=jnp.int32)

    def per_expert(carry, expert):
        dx_acc, dgate_acc = carry
        chosen = expert_ids == expert
        member = jnp.any(chosen, axis=1)
        weight = jnp.sum(jnp.where(chosen, gate_all, 0.0), axis=1)
        ranking = jnp.cumsum(member.astype(jnp.int32)) - 1
        target = jnp.where(member, ranking, slots).astype(jnp.int32)
        index = jnp.zeros((slots + 1,), jnp.int32).at[target].set(positions)[:slots]
        valid = jnp.zeros((slots + 1,), jnp.float32).at[target].set(1.0)[:slots]
        rows_in = tokens[index]
        rows_grad = grad_out[index]
        row_weight = (weight[index] * valid)[:, None]
        node = expert // E_NODE
        column = (expert % E_NODE) * FF
        gate_w = lax.dynamic_slice_in_dim(lax.dynamic_index_in_dim(w_gate, node, 0, keepdims=False), column, FF, 1)
        up_w = lax.dynamic_slice_in_dim(lax.dynamic_index_in_dim(w_up, node, 0, keepdims=False), column, FF, 1)
        down_w = lax.dynamic_slice_in_dim(lax.dynamic_index_in_dim(w_down, node, 0, keepdims=False), column, FF, 1)
        grad_gate, grad_up, weighted, product = ffn_backward(rows_in, rows_grad, row_weight, gate_w, up_w, down_w)
        partial_value = block_rows(grad_gate, grad_up, gate_w, up_w, ff_block)
        stat = block_stat(product, ff_block)
        dx_acc = dx_acc.at[index].add(partial_value * valid[:, None])
        token_stat = jnp.zeros((n_tok,), jnp.float32).at[index].add(stat * valid)
        dgate_acc = dgate_acc + jnp.where(chosen, token_stat[:, None], 0.0)
        grads = (contract_first(rows_in, grad_gate).astype(jnp.bfloat16), contract_first(rows_in, grad_up).astype(jnp.bfloat16), contract_first(rows_grad, weighted).astype(jnp.bfloat16))
        return (dx_acc, dgate_acc), grads

    start_carry = (jnp.zeros((n_tok, width), jnp.float32), jnp.zeros(expert_ids.shape, jnp.float32))
    (dx_routed, dgates), stacked = lax.scan(per_expert, start_carry, jnp.arange(E_NODE * N_NODE, dtype=jnp.int32))

    def arrange(grad):
        shaped = grad.reshape(N_NODE, E_NODE, width, FF)
        return jnp.transpose(shaped, (0, 2, 1, 3)).reshape(N_NODE, width, E_NODE * FF)

    unit_weight = jnp.ones((n_tok, 1), jnp.float32)
    grad_gate, grad_up, weighted, product = ffn_backward(tokens, grad_out, unit_weight, s_gate, s_up, s_down)
    dx_shared = block_rows(grad_gate, grad_up, s_gate, s_up, FFS // N_LOCAL)
    per_node = n_tok // N_NODE

    def node_step(index, totals):
        start = index * per_node
        rows_in = lax.dynamic_slice_in_dim(tokens, start, per_node, 0)
        rows_grad = lax.dynamic_slice_in_dim(grad_out, start, per_node, 0)
        parts = (contract_first(rows_in, lax.dynamic_slice_in_dim(grad_gate, start, per_node, 0)), contract_first(rows_in, lax.dynamic_slice_in_dim(grad_up, start, per_node, 0)), contract_first(rows_grad, lax.dynamic_slice_in_dim(weighted, start, per_node, 0)))
        return tuple(total + lax.optimization_barrier(part.astype(jnp.bfloat16)).astype(jnp.float32) for total, part in zip(totals, parts))

    empty = jnp.zeros((width, FFS), jnp.float32)
    shared = lax.fori_loop(0, N_NODE, node_step, (empty, empty, empty))
    dx = (dx_routed + dx_shared).astype(jnp.bfloat16)
    return (dx, dgates, arrange(stacked[0]), arrange(stacked[1]), arrange(stacked[2]), shared[0].astype(jnp.bfloat16), shared[1].astype(jnp.bfloat16), shared[2].astype(jnp.bfloat16))
```

```python
import jax
import jax.numpy as jnp
from jax import lax
from jax.experimental import pallas as pl
from jax.experimental.pallas import tpu as pltpu
from jax.sharding import PartitionSpec as P

MESH = pl.DeviceIdType.MESH
F32 = jnp.float32
BF16 = jnp.bfloat16
UNIT = 128
ROWS = 16
RING = 4


def dot(a, b, ca, cb):
    return lax.dot_general(a, b, (((ca,), (cb,)), ((), ())), preferred_element_type=F32)


def body(
    h_ref, wg_ref, wu_ref, wd_ref, sg_ref, su_ref, sd_ref,
    ret_ref, dwg_ref, dwu_ref, dwd_ref, dsg_ref, dsu_ref, dsd_ref,
    tt, tg, xx, w_all, v_all, gg, acc_p, acc_u,
    r1, r2, q1, q2, sw, pw, z1, z2, dw, out, ds,
    send_sem, recv_sem, load_sem, store_sem,
):
    width = wg_ref.shape[1]
    wide = width + UNIT
    block = width // 8
    half_block = block // 2
    node, here = lax.axis_index("node"), lax.axis_index("local")
    z, core = node // 2, node % 2
    y, x = here // RING, here % RING

    def step(v, by):
        return (v + by) % RING

    x_plus, x_minus = (node, y * RING + step(x, 1)), (node, y * RING + step(x, 3))
    y_plus, y_minus = (node, step(y, 1) * RING + x), (node, step(y, 3) * RING + x)
    z_plus, z_minus = (step(z, 1) * 2 + core, here), (step(z, 3) * 2 + core, here)
    partner = (z * 2 + (1 - core), here)
    first = ((x_plus, x_minus), (y_plus, y_minus))
    second = ((y_plus, y_minus), (x_plus, x_minus))

    loads = []

    def load(src, dst):
        copy = pltpu.make_async_copy(src, dst, load_sem.at[len(loads)])
        copy.start()
        loads.append(copy)

    for h in range(2):
        load(h_ref.at[h, :, pl.ds(0, wide)], tt.at[h, 0, 0])
        load(h_ref.at[h, :, pl.ds(wide, width)], tg.at[h, 0, 0])
    for i, ref in enumerate((wg_ref.at[0], wu_ref.at[0], sg_ref, su_ref)):
        load(ref, w_all.at[:, pl.ds(i * UNIT, UNIT)])
    for i, ref in enumerate((wd_ref.at[0], sd_ref)):
        load(ref, v_all.at[:, pl.ds(i * UNIT, UNIT)])

    barrier = pltpu.get_barrier_semaphore()
    for device in (x_plus, x_minus, y_plus, y_minus, z_plus, z_minus, partner):
        pl.semaphore_signal(barrier, inc=1, device_id=device, device_id_type=MESH)
    pl.semaphore_wait(barrier, 7)

    sends = []

    def send(src, dst, device):
        copy = pltpu.make_async_remote_copy(
            src_ref=src, dst_ref=dst, send_sem=send_sem.at[len(sends)],
            recv_sem=recv_sem.at[len(sends)], device_id=device, device_id_type=MESH,
        )
        copy.start()
        sends.append(copy)
        return copy

    for copy in loads[:4]:
        copy.wait()
    one = {}
    for part in range(2):
        for h in range(2):
            plus, minus = first[h]
            a, b = (tt, tg) if part == 0 else (tg, tt)
            one[h, "p", part] = send(a.at[h, 0, 0], a.at[h, 0, 3], plus)
            one[h, "m", part] = send(b.at[h, 0, 0], b.at[h, 0, 1], minus)
    far = {}
    for h in range(2):
        plus, minus = first[h]
        one[h, "p", 0].wait_recv()
        far[h, "p"] = send(tt.at[h, 0, 3], tt.at[h, 0, 2], plus)
        one[h, "m", 0].wait_recv()
        far[h, "m"] = send(tg.at[h, 0, 1], tg.at[h, 0, 2], minus)
    two = {}

    def second_hop(h, d):
        plus, minus = second[h]
        two[h, d, "pt"] = send(tt.at[h, 0, d], tt.at[h, 3, d], plus)
        two[h, d, "mg"] = send(tg.at[h, 0, d], tg.at[h, 1, d], minus)
        two[h, d, "pg"] = send(tg.at[h, 0, d], tg.at[h, 3, d], plus)
        two[h, d, "mt"] = send(tt.at[h, 0, d], tt.at[h, 1, d], minus)

    for h in range(2):
        second_hop(h, 0)
    for h in range(2):
        one[h, "p", 1].wait_recv()
        second_hop(h, 3)
    for h in range(2):
        one[h, "m", 1].wait_recv()
        second_hop(h, 1)
    for h in range(2):
        far[h, "p"].wait_recv()
        far[h, "m"].wait_recv()
        second_hop(h, 2)

    rows = 2 * RING * ROWS
    expert = here // (RING * RING // 2)
    lane = lax.broadcasted_iota(jnp.int32, (RING * ROWS, UNIT), 1)
    depth = width // 7

    def compute(i):
        acc_p[...] = jnp.zeros_like(acc_p)
        acc_u[...] = jnp.zeros_like(acc_u)

        def forward(k, carry):
            at = pl.ds(pl.multiple_of(k * depth, UNIT), depth)
            t = jnp.concatenate([tt[h, i, :, :, at].reshape(rows // 2, depth) for h in range(2)], 0)
            g = jnp.concatenate([tg[h, i, :, :, at].reshape(rows // 2, depth) for h in range(2)], 0)
            acc_p[...] += dot(t, w_all[at, :], 1, 0)
            acc_u[...] += dot(g, v_all[at, :], 1, 0)
            return carry

        lax.fori_loop(0, 7, forward, 0)
        for h in range(2):
            mine = slice(h * rows // 2, (h + 1) * rows // 2)
            side = tt[h, i, :, :, width:].reshape(rows // 2, UNIT).astype(F32)
            gate = jnp.where(expert == 0, side[:, 0:1], side[:, 1:2])
            for j, weight in enumerate((gate, side[:, 2:3])):
                pre = acc_p[mine, 2 * j * UNIT : (2 * j + 1) * UNIT]
                up = acc_p[mine, (2 * j + 1) * UNIT : (2 * j + 2) * UNIT]
                upstream = acc_u[mine, j * UNIT : (j + 1) * UNIT]
                sig = 1.0 / (1.0 + jnp.exp(-pre))
                activ = pre * sig
                slope = sig * (1.0 + pre * (1.0 - sig))
                hidden = activ * up
                scaled = weight * upstream
                for place, value in (
                    (2 * j, scaled * up * slope),
                    (2 * j + 1, scaled * activ),
                    (4 + j, weight * hidden),
                ):
                    gg[h, i, :, :, place * UNIT : (place + 1) * UNIT] = value.astype(BF16).reshape(
                        RING, ROWS, UNIT
                    )
                if j == 0:
                    score = jnp.sum(hidden * upstream, axis=1, keepdims=True)
                    xx[h, i, :, :, width:] = (
                        jnp.where(lane == expert, score, 0.0).astype(BF16).reshape(RING, ROWS, UNIT)
                    )

        def backward(k, carry):
            at = pl.ds(pl.multiple_of(k * (depth // 2), UNIT), depth // 2)
            g = jnp.concatenate(
                [gg[h, i, :, :, : 4 * UNIT].reshape(rows // 2, 4 * UNIT) for h in range(2)], 0
            )
            value = dot(g, w_all[at, :], 1, 1).astype(BF16)
            for h in range(2):
                xx[h, i, :, :, at] = value[h * rows // 2 : (h + 1) * rows // 2].reshape(
                    RING, ROWS, depth // 2
                )
            return carry

        lax.fori_loop(0, 14, backward, 0)

    for copy in loads[4:]:
        copy.wait()
    compute(0)
    onward = {}
    for d in (0, 3, 1, 2):
        for h in range(2):
            plus, minus = second[h]
            two[h, d, "pt"].wait_recv()
            onward[h, d, "p"] = send(tt.at[h, 3, d], tt.at[h, 2, d], plus)
            two[h, d, "mg"].wait_recv()
            onward[h, d, "m"] = send(tg.at[h, 1, d], tg.at[h, 2, d], minus)
    for d in range(RING):
        for h in range(2):
            two[h, d, "pg"].wait_recv()
            two[h, d, "mt"].wait_recv()
    compute(1)
    compute(3)
    for copy in onward.values():
        copy.wait_recv()
    compute(2)

    upper, lower = (2, 1), (3, 0)
    back = {}
    for h in range(2):
        plus, minus = second[h]
        for j in range(2):
            back[h, "p", j] = send(xx.at[h, 2, upper[j]], r1.at[h, 0, j], plus)
            back[h, "m", j] = send(xx.at[h, 2, lower[j]], r1.at[h, 1, j], minus)
    full = {}
    for h in range(2):
        plus, minus = second[h]
        for j in range(2):
            full[h, "p", lower[j]] = send(xx.at[h, 1, lower[j]], r2.at[h, 0, lower[j]], plus)
            full[h, "m", upper[j]] = send(xx.at[h, 3, upper[j]], r2.at[h, 1, upper[j]], minus)

    stores = []

    def store(src, dst):
        copy = pltpu.make_async_copy(src, dst, store_sem.at[len(stores)])
        copy.start()
        stores.append(copy)

    everything = 2 * RING * RING * ROWS

    def weights(parity):
        def one_block(k, carry):
            b = 2 * k + parity
            at = pl.ds(pl.multiple_of(b * block, UNIT), block)
            t = tt[:, :, :, :, at].reshape(everything, block)
            g = tg[:, :, :, :, at].reshape(everything, block)
            a = dot(t, gg[:, :, :, :, : 4 * UNIT].reshape(everything, 4 * UNIT), 0, 0)
            c = dot(g, gg[:, :, :, :, 4 * UNIT :].reshape(everything, 2 * UNIT), 0, 0)
            dw[0, b] = a[:, :UNIT].astype(BF16)
            dw[1, b] = a[:, UNIT : 2 * UNIT].astype(BF16)
            dw[2, b] = c[:, :UNIT].astype(BF16)
            sw[parity, k, :, : 2 * UNIT] = a[:, 2 * UNIT :].astype(BF16)
            sw[parity, k, :, 2 * UNIT :] = c[:, UNIT:].astype(BF16)
            return carry

        lax.fori_loop(0, RING, one_block, 0)

    def add(dst, *srcs):
        total = dst[...].astype(F32)
        for src in srcs:
            total = total + src[...].astype(F32)
        dst[...] = total.astype(BF16)

    weights(1 - core)
    swap = send(sw.at[1 - core], pw, partner)
    for j in range(2):
        for h in range(2):
            plus, minus = second[h]
            back[h, "p", j].wait_recv()
            add(xx.at[h, 1, upper[j]], r1.at[h, 0, j])
            full[h, "p", upper[j]] = send(xx.at[h, 1, upper[j]], r2.at[h, 0, upper[j]], plus)
            back[h, "m", j].wait_recv()
            add(xx.at[h, 3, lower[j]], r1.at[h, 1, j])
            full[h, "m", lower[j]] = send(xx.at[h, 3, lower[j]], r2.at[h, 1, lower[j]], minus)
    weights(core)
    for b in range(8):
        for j, ref in enumerate((dwg_ref, dwu_ref, dwd_ref)):
            store(dw.at[j, b], ref.at[0, pl.ds(b * block, block)])
    swap.wait_recv()

    def add_swap(k, carry):
        add(sw.at[core, k], pw.at[k])
        return carry

    lax.fori_loop(0, RING, add_swap, 0)
    low, high = pl.ds(0, half_block), pl.ds(half_block, half_block)
    z_back = (
        send(sw.at[core, step(z, 2), low], z1.at[0], z_plus),
        send(sw.at[core, step(z, 2), high], z1.at[1], z_minus),
    )
    z_full = [
        send(sw.at[core, step(z, 1), high], z2.at[0, high], z_plus),
        send(sw.at[core, step(z, 3), low], z2.at[1, low], z_minus),
    ]

    cut = (wide // UNIT + 1) // 2 * UNIT
    left, right = pl.ds(0, cut), pl.ds(cut, wide - cut)
    for d in (2, 3, 1, 0):
        for h in range(2):
            full[h, "p", d].wait_recv()
            full[h, "m", d].wait_recv()
            add(xx.at[h, 0, d], r2.at[h, 0, d], r2.at[h, 1, d])
            plus, minus = first[h]
            if d == 2:
                back[h, "P"] = send(xx.at[h, 0, 2, :, left], q1.at[h, 0, :, left], plus)
                back[h, "M"] = send(xx.at[h, 0, 2, :, right], q1.at[h, 1, :, right], minus)
            if d == 1:
                full[h, "P"] = send(xx.at[h, 0, 1, :, right], q2.at[h, 0, :, right], plus)
            if d == 3:
                full[h, "M"] = send(xx.at[h, 0, 3, :, left], q2.at[h, 1, :, left], minus)
    z_back[0].wait_recv()
    add(sw.at[core, step(z, 1), low], z1.at[0])
    z_full.append(send(sw.at[core, step(z, 1), low], z2.at[0, low], z_plus))
    z_back[1].wait_recv()
    add(sw.at[core, step(z, 3), high], z1.at[1])
    z_full.append(send(sw.at[core, step(z, 3), high], z2.at[1, high], z_minus))
    last = []
    for h in range(2):
        plus, minus = first[h]
        back[h, "P"].wait_recv()
        add(xx.at[h, 0, 1, :, left], q1.at[h, 0, :, left])
        last.append(send(xx.at[h, 0, 1, :, left], q2.at[h, 0, :, left], plus))
        back[h, "M"].wait_recv()
        add(xx.at[h, 0, 3, :, right], q1.at[h, 1, :, right])
        last.append(send(xx.at[h, 0, 3, :, right], q2.at[h, 1, :, right], minus))
    for copy in last:
        copy.wait_recv()
    for h in range(2):
        full[h, "P"].wait_recv()
        full[h, "M"].wait_recv()
        total = xx[h, 0, 0].astype(F32) + q2[h, 0].astype(F32) + q2[h, 1].astype(F32)
        out[h] = total.astype(BF16)
    store(out, ret_ref)
    for copy in z_full:
        copy.wait_recv()
    total = sw[core, z].astype(F32) + z2[0].astype(F32) + z2[1].astype(F32)
    for j, ref in enumerate((dsg_ref, dsu_ref, dsd_ref)):
        ds[j] = total[:, j * UNIT : (j + 1) * UNIT].astype(BF16)
        store(ds.at[j], ref)
    for copy in sends:
        copy.wait_send()
    for copy in stores:
        copy.wait()


SENDS = 8 + 4 + 32 + 16 + 8 + 8 + 8 + 1 + 6 + 4 * 2 + 4


def expert_layer(rows, w_gate, w_up, w_down, s_gate, s_up, s_down):
    width = s_gate.shape[0]
    wide = width + UNIT
    block = width // 8
    shape = jax.ShapeDtypeStruct
    return pl.pallas_call(
        body,
        out_shape=(
            shape((2, ROWS, wide), BF16),
            *(shape(w_gate.shape, BF16) for _ in range(3)),
            *(shape((block, UNIT), BF16) for _ in range(3)),
        ),
        in_specs=[pl.BlockSpec(memory_space=pl.ANY)] * 7,
        out_specs=(pl.BlockSpec(memory_space=pl.ANY),) * 7,
        scratch_shapes=[
            pltpu.VMEM((2, RING, RING, ROWS, wide), BF16),
            pltpu.VMEM((2, RING, RING, ROWS, width), BF16),
            pltpu.VMEM((2, RING, RING, ROWS, wide), BF16),
            pltpu.VMEM((width, 4 * UNIT), BF16),
            pltpu.VMEM((width, 2 * UNIT), BF16),
            pltpu.VMEM((2, RING, RING, ROWS, 6 * UNIT), BF16),
            pltpu.VMEM((2 * RING * ROWS, 4 * UNIT), F32),
            pltpu.VMEM((2 * RING * ROWS, 2 * UNIT), F32),
            pltpu.VMEM((2, 2, 2, ROWS, wide), BF16),
            pltpu.VMEM((2, 2, RING, ROWS, wide), BF16),
            pltpu.VMEM((2, 2, ROWS, wide), BF16),
            pltpu.VMEM((2, 2, ROWS, wide), BF16),
            pltpu.VMEM((2, RING, block, 3 * UNIT), BF16),
            pltpu.VMEM((RING, block, 3 * UNIT), BF16),
            pltpu.VMEM((2, block // 2, 3 * UNIT), BF16),
            pltpu.VMEM((2, block, 3 * UNIT), BF16),
            pltpu.VMEM((3, 8, block, UNIT), BF16),
            pltpu.VMEM((2, ROWS, wide), BF16),
            pltpu.VMEM((3, block, UNIT), BF16),
            pltpu.SemaphoreType.DMA((SENDS,)),
            pltpu.SemaphoreType.DMA((SENDS,)),
            pltpu.SemaphoreType.DMA((10,)),
            pltpu.SemaphoreType.DMA((28,)),
        ],
        compiler_params=pltpu.CompilerParams(
            collective_id=0, has_side_effects=True, vmem_limit_bytes=67043328
        ),
    )(rows, w_gate, w_up, w_down, s_gate, s_up, s_down)


def local(tokens, grad_out, gates, expert_ids, w_gate, w_up, w_down, s_gate, s_up, s_down):
    count, width = tokens.shape
    nodes = lax.axis_size("node")
    slots = 2 * count // nodes
    places = jnp.arange(slots, dtype=jnp.int32)
    pair = 2 * jnp.arange(nodes, dtype=jnp.int32)[None, :]
    chosen = [expert_ids[:, :, None] == (pair + e)[:, None, :] for e in range(2)]
    gate = gates.astype(F32)[:, :, None]
    weight = [jnp.sum(jnp.where(c, gate, 0.0), axis=1) for c in chosen]
    named = [jnp.any(c, axis=1) for c in chosen]
    member = named[0] | named[1]
    both = (named[0] & named[1]).astype(F32)
    ranking = jnp.cumsum(member.astype(jnp.int32), axis=0) - 1
    pick = (member[:, :, None] & (ranking[:, :, None] == places)).astype(BF16)
    side = jnp.stack([weight[0], weight[1], both], axis=-1)
    side = jnp.sum(pick.astype(F32)[..., None] * side[:, :, None, :], axis=0)
    side = jnp.pad(side, ((0, 0), (0, 0), (0, UNIT - 3))).astype(BF16)
    pieces = [
        jnp.einsum("tns,td->nsd", pick, value, preferred_element_type=F32).astype(BF16)
        for value in (tokens, grad_out)
    ]
    rows = jnp.concatenate([pieces[0], side, pieces[1]], axis=2)
    rows = lax.all_to_all(rows, "node", split_axis=0, concat_axis=0, tiled=True)
    rows = rows.reshape(2, ROWS, rows.shape[2])
    ret, dwg, dwu, dwd, dsg, dsu, dsd = expert_layer(
        rows, w_gate, w_up, w_down, s_gate, s_up, s_down
    )
    ret = ret.reshape(nodes, slots, ret.shape[2])
    ret = lax.all_to_all(ret, "node", split_axis=0, concat_axis=0, tiled=True)
    dx = jnp.einsum("tns,nsd->td", pick, ret[:, :, :width], preferred_element_type=F32)
    score = ret[:, :, width : width + 2].astype(F32)
    score = jnp.sum(pick.astype(F32)[..., None] * score[None], axis=2)
    dgates = sum(
        jnp.sum(jnp.where(chosen[e], score[:, None, :, e], 0.0), axis=2) for e in range(2)
    )
    return dx.astype(BF16), dgates, dwg, dwu, dwd, dsg, dsu, dsd


def solution(mesh):
    flat = P(("node", "local"), None)
    routed = P("node", None, "local")
    shared = P(None, "local")
    return jax.shard_map(
        local,
        mesh=mesh,
        in_specs=(flat,) * 4 + (routed,) * 3 + (shared,) * 3,
        out_specs=(flat, flat) + (routed,) * 3 + (P("node", "local"),) * 3,
        check_vma=False,
    )
```

```python
import jax
import jax.numpy as jnp
from jax import lax
from jax.experimental import pallas as pl
from jax.experimental.pallas import tpu as pltpu
from jax.sharding import PartitionSpec as P

MESH = pl.DeviceIdType.MESH
F32 = jnp.float32
BF16 = jnp.bfloat16
UNIT = 128
ROWS = 16
RING = 4


def dot(a, b, ca, cb):
    return lax.dot_general(a, b, (((ca,), (cb,)), ((), ())), preferred_element_type=F32)


def body(
    tok_ref, grad_ref, gate_ref, id_ref, wg_ref, wu_ref, wd_ref, sg_ref, su_ref, sd_ref,
    dx_ref, dgate_ref, dwg_ref, dwu_ref, dwd_ref, dsg_ref, dsu_ref, dsd_ref,
    given, outgo, income, relay, answer, reply, relay_back, tt, tg, xx, w_all, v_all, gg, acc_p, acc_u,
    r1, r2, q1, q2, sw, pw, z1, z2, dw, ds,
    send_sem, recv_sem, load_sem, store_sem,
):
    width = wg_ref.shape[1]
    wide = width + UNIT
    block = width // 8
    half_block = block // 2
    node, here = lax.axis_index("node"), lax.axis_index("local")
    z, core = node // 2, node % 2
    y, x = here // RING, here % RING

    def step(v, by):
        return (v + by) % RING

    x_plus, x_minus = (node, y * RING + step(x, 1)), (node, y * RING + step(x, 3))
    y_plus, y_minus = (node, step(y, 1) * RING + x), (node, step(y, 3) * RING + x)
    z_plus, z_minus = (step(z, 1) * 2 + core, here), (step(z, 3) * 2 + core, here)
    partner = (z * 2 + (1 - core), here)
    z_plus_other = (step(z, 1) * 2 + (1 - core), here)
    z_minus_other = (step(z, 3) * 2 + (1 - core), here)
    first = ((x_plus, x_minus), (y_plus, y_minus))
    second = ((y_plus, y_minus), (x_plus, x_minus))

    loads = []

    def load(src, dst):
        copy = pltpu.make_async_copy(src, dst, load_sem.at[len(loads)])
        copy.start()
        loads.append(copy)

    load(tok_ref, given.at[0])
    load(grad_ref, given.at[1])
    for i, ref in enumerate((wg_ref.at[0], wu_ref.at[0], sg_ref, su_ref)):
        load(ref, w_all.at[:, pl.ds(i * UNIT, UNIT)])
    for i, ref in enumerate((wd_ref.at[0], sd_ref)):
        load(ref, v_all.at[:, pl.ds(i * UNIT, UNIT)])

    barrier = pltpu.get_barrier_semaphore()
    for device in (
        x_plus, x_minus, y_plus, y_minus, z_plus, z_minus, z_plus_other, z_minus_other, partner
    ):
        pl.semaphore_signal(barrier, inc=1, device_id=device, device_id_type=MESH)

    count = ROWS
    eye = lax.broadcasted_iota(jnp.int32, (count, count), 0) == lax.broadcasted_iota(
        jnp.int32, (count, count), 1
    )

    def as_row(column):
        return jnp.sum(jnp.where(eye, column, 0.0), axis=0, keepdims=True)

    def as_column(row):
        return jnp.sum(jnp.where(eye, row, 0.0), axis=1, keepdims=True)

    slot_row = lax.broadcasted_iota(jnp.int32, (2 * ROWS, count), 0)
    slot_node = ((z + (slot_row >> 3)) & 3) * 2 + ((core + (slot_row >> 2)) & 1)
    ids = id_ref[...].astype(F32)
    gates = gate_ref[...].astype(F32)
    id_rows = [as_row(ids[:, k : k + 1]) for k in range(3)]
    gate_rows = [as_row(gates[:, k : k + 1]) for k in range(3)]
    names = [
        [(id_rows[k] == (2 * slot_node + e).astype(F32)).astype(F32) for k in range(3)]
        for e in range(2)
    ]
    named = [names[e][0] + names[e][1] + names[e][2] for e in range(2)]
    member = jnp.maximum(named[0], named[1])
    earlier = (
        lax.broadcasted_iota(jnp.int32, (count, count), 0)
        < lax.broadcasted_iota(jnp.int32, (count, count), 1)
    ).astype(BF16)
    ranking = dot(member.astype(BF16), earlier, 1, 0)
    pick = jnp.where(ranking == (slot_row & 3).astype(F32), member, 0.0)
    pick_bf16 = pick.astype(BF16)
    side = [
        jnp.sum(pick * sum(names[e][k] * gate_rows[k] for k in range(3)), axis=1, keepdims=True)
        for e in range(2)
    ]
    side.append(jnp.sum(pick * named[0] * named[1], axis=1, keepdims=True))
    slot_lane = lax.broadcasted_iota(jnp.int32, (2 * ROWS, UNIT), 1)
    columns = sum(jnp.where(slot_lane == i, side[i], 0.0) for i in range(3)).astype(BF16)
    for s in range(8):
        outgo[s, :, width:wide] = columns[4 * s : 4 * s + 4]
    for copy in loads[:2]:
        copy.wait()
    stretch = width // 7

    def cut_rows(k, carry):
        at = pl.multiple_of(k * stretch, UNIT)
        for i, offset in enumerate((0, wide)):
            value = dot(pick_bf16, given[i, :, pl.ds(at, stretch)], 1, 0)
            for s in range(8):
                outgo[s, :, pl.ds(pl.multiple_of(at + offset, UNIT), stretch)] = value[
                    4 * s : 4 * s + 4
                ].astype(BF16)
        return carry

    lax.fori_loop(0, 7, cut_rows, 0)
    pl.semaphore_wait(barrier, 9)

    sends = []

    def send(src, dst, device):
        copy = pltpu.make_async_remote_copy(
            src_ref=src, dst_ref=dst, send_sem=send_sem.at[len(sends)],
            recv_sem=recv_sem.at[len(sends)], device_id=device, device_id_type=MESH,
        )
        copy.start()
        sends.append(copy)
        return copy

    across = {
        (0, 1): send(outgo.at[1], income.at[1], partner),
        (3, 0): send(outgo.at[6], income.at[2], z_minus),
        (2, 0): send(outgo.at[4], relay.at[0], z_plus),
        (3, 1): send(outgo.at[7], income.at[3], z_minus_other),
        (1, 0): send(outgo.at[2], income.at[6], z_plus),
        (2, 1): send(outgo.at[5], relay.at[1], z_minus),
        (1, 1): send(outgo.at[3], income.at[7], z_plus_other),
    }

    def stack(h):
        def piece(at, size):
            return jnp.concatenate(
                [
                    (outgo if h == 0 and s == 0 else income)[4 * h + s, :, pl.ds(at, size)].astype(F32)
                    for s in range(4)
                ],
                0,
            ).astype(BF16)

        def one_stretch(k, carry):
            at = pl.multiple_of(k * stretch, UNIT)
            tt[h, 0, 0, :, pl.ds(at, stretch)] = piece(at, stretch)
            tg[h, 0, 0, :, pl.ds(at, stretch)] = piece(pl.multiple_of(at + wide, UNIT), stretch)
            return carry

        lax.fori_loop(0, 7, one_stretch, 0)
        tt[h, 0, 0, :, width:] = piece(width, UNIT)

    one, two, far = {}, {}, {}

    def first_hop(h):
        plus, minus = first[h]
        for part, (a, b) in enumerate(((tt, tg), (tg, tt))):
            one[h, "p", part] = send(a.at[h, 0, 0], a.at[h, 0, 3], plus)
            one[h, "m", part] = send(b.at[h, 0, 0], b.at[h, 0, 1], minus)

    across[2, 0].wait_recv()
    forth = [send(relay.at[0], income.at[4], z_plus)]
    for key in ((0, 1), (3, 0), (3, 1)):
        across[key].wait_recv()
    stack(0)
    first_hop(0)
    across[2, 1].wait_recv()
    forth.append(send(relay.at[1], income.at[5], z_minus_other))

    def second_hop(h, d):
        plus, minus = second[h]
        two[h, d, "pt"] = send(tt.at[h, 0, d], tt.at[h, 3, d], plus)
        two[h, d, "mg"] = send(tg.at[h, 0, d], tg.at[h, 1, d], minus)
        two[h, d, "pg"] = send(tg.at[h, 0, d], tg.at[h, 3, d], plus)
        two[h, d, "mt"] = send(tt.at[h, 0, d], tt.at[h, 1, d], minus)

    def pass_on(h):
        plus, minus = first[h]
        one[h, "p", 0].wait_recv()
        far[h, "p"] = send(tt.at[h, 0, 3], tt.at[h, 0, 2], plus)
        one[h, "m", 0].wait_recv()
        far[h, "m"] = send(tg.at[h, 0, 1], tg.at[h, 0, 2], minus)

    second_hop(0, 0)
    for copy in (across[1, 0], across[1, 1], *forth):
        copy.wait_recv()
    stack(1)
    first_hop(1)
    pass_on(0)
    second_hop(1, 0)
    pass_on(1)
    for h in range(2):
        one[h, "p", 1].wait_recv()
        second_hop(h, 3)
    for h in range(2):
        one[h, "m", 1].wait_recv()
        second_hop(h, 1)
    for h in range(2):
        far[h, "p"].wait_recv()
        far[h, "m"].wait_recv()
        second_hop(h, 2)

    rows = 2 * RING * ROWS
    expert = here // (RING * RING // 2)
    lane = lax.broadcasted_iota(jnp.int32, (RING * ROWS, UNIT), 1)
    depth = width // 7

    def compute(i):
        acc_p[...] = jnp.zeros_like(acc_p)
        acc_u[...] = jnp.zeros_like(acc_u)

        def forward(k, carry):
            at = pl.ds(pl.multiple_of(k * depth, UNIT), depth)
            t = jnp.concatenate([tt[h, i, :, :, at].reshape(rows // 2, depth) for h in range(2)], 0)
            g = jnp.concatenate([tg[h, i, :, :, at].reshape(rows // 2, depth) for h in range(2)], 0)
            acc_p[...] += dot(t, w_all[at, :], 1, 0)
            acc_u[...] += dot(g, v_all[at, :], 1, 0)
            return carry

        lax.fori_loop(0, 7, forward, 0)
        for h in range(2):
            mine = slice(h * rows // 2, (h + 1) * rows // 2)
            side = tt[h, i, :, :, width:].reshape(rows // 2, UNIT).astype(F32)
            gate = jnp.where(expert == 0, side[:, 0:1], side[:, 1:2])
            for j, weight in enumerate((gate, side[:, 2:3])):
                pre = acc_p[mine, 2 * j * UNIT : (2 * j + 1) * UNIT]
                up = acc_p[mine, (2 * j + 1) * UNIT : (2 * j + 2) * UNIT]
                upstream = acc_u[mine, j * UNIT : (j + 1) * UNIT]
                sig = 1.0 / (1.0 + jnp.exp(-pre))
                activ = pre * sig
                slope = sig * (1.0 + pre * (1.0 - sig))
                hidden = activ * up
                scaled = weight * upstream
                for place, value in (
                    (2 * j, scaled * up * slope),
                    (2 * j + 1, scaled * activ),
                    (4 + j, weight * hidden),
                ):
                    gg[h, i, :, :, place * UNIT : (place + 1) * UNIT] = value.astype(BF16).reshape(
                        RING, ROWS, UNIT
                    )
                if j == 0:
                    score = jnp.sum(hidden * upstream, axis=1, keepdims=True)
                    xx[h, i, :, :, width:] = (
                        jnp.where(lane == expert, score, 0.0).astype(BF16).reshape(RING, ROWS, UNIT)
                    )

        def backward(k, carry):
            at = pl.ds(pl.multiple_of(k * (depth // 2), UNIT), depth // 2)
            g = jnp.concatenate(
                [gg[h, i, :, :, : 4 * UNIT].reshape(rows // 2, 4 * UNIT) for h in range(2)], 0
            )
            value = dot(g, w_all[at, :], 1, 1).astype(BF16)
            for h in range(2):
                xx[h, i, :, :, at] = value[h * rows // 2 : (h + 1) * rows // 2].reshape(
                    RING, ROWS, depth // 2
                )
            return carry

        lax.fori_loop(0, 14, backward, 0)

    for copy in loads[2:]:
        copy.wait()
    compute(0)
    onward = {}
    for d in (0, 3, 1, 2):
        for h in range(2):
            plus, minus = second[h]
            two[h, d, "pt"].wait_recv()
            onward[h, d, "p"] = send(tt.at[h, 3, d], tt.at[h, 2, d], plus)
            two[h, d, "mg"].wait_recv()
            onward[h, d, "m"] = send(tg.at[h, 1, d], tg.at[h, 2, d], minus)
    for d in range(RING):
        for h in range(2):
            two[h, d, "pg"].wait_recv()
            two[h, d, "mt"].wait_recv()
    compute(1)
    compute(3)
    upper, lower = (2, 1), (3, 0)
    full = {}
    for h in range(2):
        plus, minus = second[h]
        for j in range(2):
            full[h, "p", lower[j]] = send(xx.at[h, 1, lower[j]], r2.at[h, 0, lower[j]], plus)
            full[h, "m", upper[j]] = send(xx.at[h, 3, upper[j]], r2.at[h, 1, upper[j]], minus)
    for copy in onward.values():
        copy.wait_recv()
    compute(2)
    back = {}
    for j in range(2):
        for h in range(2):
            plus, minus = second[h]
            back[h, "p", j] = send(xx.at[h, 2, upper[j]], r1.at[h, 0, j], plus)
            back[h, "m", j] = send(xx.at[h, 2, lower[j]], r1.at[h, 1, j], minus)

    stores = []

    def store(src, dst):
        copy = pltpu.make_async_copy(src, dst, store_sem.at[len(stores)])
        copy.start()
        stores.append(copy)

    everything = 2 * RING * RING * ROWS

    def weights(parity):
        def one_block(k, carry):
            b = 2 * k + parity
            at = pl.ds(pl.multiple_of(b * block, UNIT), block)
            t = tt[:, :, :, :, at].reshape(everything, block)
            g = tg[:, :, :, :, at].reshape(everything, block)
            a = dot(t, gg[:, :, :, :, : 4 * UNIT].reshape(everything, 4 * UNIT), 0, 0)
            c = dot(g, gg[:, :, :, :, 4 * UNIT :].reshape(everything, 2 * UNIT), 0, 0)
            dw[0, b] = a[:, :UNIT].astype(BF16)
            dw[1, b] = a[:, UNIT : 2 * UNIT].astype(BF16)
            dw[2, b] = c[:, :UNIT].astype(BF16)
            sw[parity, k, :, : 2 * UNIT] = a[:, 2 * UNIT :].astype(BF16)
            sw[parity, k, :, 2 * UNIT :] = c[:, UNIT:].astype(BF16)
            return carry

        lax.fori_loop(0, RING, one_block, 0)

    def add(dst, *srcs):
        total = dst[...].astype(F32)
        for src in srcs:
            total = total + src[...].astype(F32)
        dst[...] = total.astype(BF16)

    weights(1 - core)
    swap = send(sw.at[1 - core], pw, partner)
    for j in range(2):
        for h in range(2):
            plus, minus = second[h]
            back[h, "p", j].wait_recv()
            add(xx.at[h, 1, upper[j]], r1.at[h, 0, j])
            full[h, "p", upper[j]] = send(xx.at[h, 1, upper[j]], r2.at[h, 0, upper[j]], plus)
            back[h, "m", j].wait_recv()
            add(xx.at[h, 3, lower[j]], r1.at[h, 1, j])
            full[h, "m", lower[j]] = send(xx.at[h, 3, lower[j]], r2.at[h, 1, lower[j]], minus)
    weights(core)
    for b in range(8):
        for j, ref in enumerate((dwg_ref, dwu_ref, dwd_ref)):
            store(dw.at[j, b], ref.at[0, pl.ds(b * block, block)])
    swap.wait_recv()

    def add_swap(k, carry):
        add(sw.at[core, k], pw.at[k])
        return carry

    lax.fori_loop(0, RING, add_swap, 0)
    low, high = pl.ds(0, half_block), pl.ds(half_block, half_block)
    z_back = (
        send(sw.at[core, step(z, 2), low], z1.at[0], z_plus),
        send(sw.at[core, step(z, 2), high], z1.at[1], z_minus),
    )
    z_full = [
        send(sw.at[core, step(z, 1), high], z2.at[0, high], z_plus),
        send(sw.at[core, step(z, 3), low], z2.at[1, low], z_minus),
    ]

    cut = (wide // UNIT + 1) // 2 * UNIT
    left, right = pl.ds(0, cut), pl.ds(cut, wide - cut)
    for d in (2, 3, 1, 0):
        for h in range(2):
            full[h, "p", d].wait_recv()
            full[h, "m", d].wait_recv()
            add(xx.at[h, 0, d], r2.at[h, 0, d], r2.at[h, 1, d])
            plus, minus = first[h]
            if d == 2:
                back[h, "P"] = send(xx.at[h, 0, 2, :, left], q1.at[h, 0, :, left], plus)
                back[h, "M"] = send(xx.at[h, 0, 2, :, right], q1.at[h, 1, :, right], minus)
            if d == 1:
                full[h, "P"] = send(xx.at[h, 0, 1, :, right], q2.at[h, 0, :, right], plus)
            if d == 3:
                full[h, "M"] = send(xx.at[h, 0, 3, :, left], q2.at[h, 1, :, left], minus)
    z_back[0].wait_recv()
    add(sw.at[core, step(z, 1), low], z1.at[0])
    z_full.append(send(sw.at[core, step(z, 1), low], z2.at[0, low], z_plus))
    z_back[1].wait_recv()
    add(sw.at[core, step(z, 3), high], z1.at[1])
    z_full.append(send(sw.at[core, step(z, 3), high], z2.at[1, high], z_minus))
    last = []
    for h in range(2):
        plus, minus = first[h]
        back[h, "P"].wait_recv()
        add(xx.at[h, 0, 1, :, left], q1.at[h, 0, :, left])
        last.append(send(xx.at[h, 0, 1, :, left], q2.at[h, 0, :, left], plus))
        back[h, "M"].wait_recv()
        add(xx.at[h, 0, 3, :, right], q1.at[h, 1, :, right])
        last.append(send(xx.at[h, 0, 3, :, right], q2.at[h, 1, :, right], minus))
    for h in range(2):
        full[h, "P"].wait_recv()
        full[h, "M"].wait_recv()
        last[2 * h].wait_recv()
        last[2 * h + 1].wait_recv()

        def one_stretch(k, carry, h=h):
            at = pl.ds(pl.multiple_of(k * 3 * UNIT, UNIT), 3 * UNIT)
            total = xx[h, 0, 0, :, at].astype(F32)
            for i in range(2):
                total = total + q2[h, i, :, at].astype(F32)
            for s in range(4):
                answer[4 * h + s, :, at] = total[4 * s : 4 * s + 4].astype(BF16)
            return carry

        lax.fori_loop(0, wide // (3 * UNIT), one_stretch, 0)
        if h == 0:
            home = [
                send(answer.at[2], reply.at[6], z_plus),
                send(answer.at[3], reply.at[7], z_plus_other),
                send(answer.at[1], reply.at[1], partner),
            ]
        else:
            home += [
                send(answer.at[4], relay_back.at[0], z_plus),
                send(answer.at[5], relay_back.at[1], z_minus),
                send(answer.at[6], reply.at[2], z_minus),
                send(answer.at[7], reply.at[3], z_minus_other),
            ]
    for copy in z_full:
        copy.wait_recv()
    total = sw[core, z].astype(F32) + z2[0].astype(F32) + z2[1].astype(F32)
    for j, ref in enumerate((dsg_ref, dsu_ref, dsd_ref)):
        ds[j] = total[:, j * UNIT : (j + 1) * UNIT].astype(BF16)
        store(ds.at[j], ref)
    home[3].wait_recv()
    home.append(send(relay_back.at[0], reply.at[4], z_plus))
    home[4].wait_recv()
    home.append(send(relay_back.at[1], reply.at[5], z_minus_other))
    for i in (0, 1, 2, 5, 6, 7, 8):
        home[i].wait_recv()

    def answers(at, size):
        return jnp.concatenate(
            [(answer if s == 0 else reply)[s, :, pl.ds(at, size)].astype(F32) for s in range(8)], 0
        )

    def finish(k, carry):
        at = pl.multiple_of(k * stretch, UNIT)
        total = dot(pick_bf16, answers(at, stretch).astype(BF16), 0, 0)
        given[0, :, pl.ds(at, stretch)] = total.astype(BF16)
        return carry

    lax.fori_loop(0, 7, finish, 0)
    store(given.at[0], dx_ref)
    score = answers(width, UNIT)
    for k in range(3):
        row = jnp.sum(
            pick * (names[0][k] * score[:, 0:1] + names[1][k] * score[:, 1:2]),
            axis=0, keepdims=True,
        )
        dgate_ref[:, k : k + 1] = as_column(row)
    for copy in sends:
        copy.wait_send()
    for copy in stores:
        copy.wait()


SENDS = 103 + 9 + 9


def expert_layer(tokens, grad_out, gates, ids, w_gate, w_up, w_down, s_gate, s_up, s_down):
    width = s_gate.shape[0]
    wide = width + UNIT
    block = width // 8
    shape = jax.ShapeDtypeStruct
    anywhere = pl.BlockSpec(memory_space=pl.ANY)
    inside = pl.BlockSpec(memory_space=pltpu.VMEM)
    return pl.pallas_call(
        body,
        out_shape=(
            shape(tokens.shape, BF16),
            shape(gates.shape, F32),
            *(shape(w_gate.shape, BF16) for _ in range(3)),
            *(shape((block, UNIT), BF16) for _ in range(3)),
        ),
        in_specs=[anywhere] * 2 + [inside] * 2 + [anywhere] * 6,
        out_specs=(anywhere, inside) + (anywhere,) * 6,
        scratch_shapes=[
            pltpu.VMEM((2, ROWS, width), BF16),
            pltpu.VMEM((8, 4, wide + width), BF16),
            pltpu.VMEM((8, 4, wide + width), BF16),
            pltpu.VMEM((2, 4, wide + width), BF16),
            pltpu.VMEM((8, 4, wide), BF16),
            pltpu.VMEM((8, 4, wide), BF16),
            pltpu.VMEM((2, 4, wide), BF16),
            pltpu.VMEM((2, RING, RING, ROWS, wide), BF16),
            pltpu.VMEM((2, RING, RING, ROWS, width), BF16),
            pltpu.VMEM((2, RING, RING, ROWS, wide), BF16),
            pltpu.VMEM((width, 4 * UNIT), BF16),
            pltpu.VMEM((width, 2 * UNIT), BF16),
            pltpu.VMEM((2, RING, RING, ROWS, 6 * UNIT), BF16),
            pltpu.VMEM((2 * RING * ROWS, 4 * UNIT), F32),
            pltpu.VMEM((2 * RING * ROWS, 2 * UNIT), F32),
            pltpu.VMEM((2, 2, 2, ROWS, wide), BF16),
            pltpu.VMEM((2, 2, RING, ROWS, wide), BF16),
            pltpu.VMEM((2, 2, ROWS, wide), BF16),
            pltpu.VMEM((2, 2, ROWS, wide), BF16),
            pltpu.VMEM((2, RING, block, 3 * UNIT), BF16),
            pltpu.VMEM((RING, block, 3 * UNIT), BF16),
            pltpu.VMEM((2, block // 2, 3 * UNIT), BF16),
            pltpu.VMEM((2, block, 3 * UNIT), BF16),
            pltpu.VMEM((3, 8, block, UNIT), BF16),
            pltpu.VMEM((3, block, UNIT), BF16),
            pltpu.SemaphoreType.DMA((SENDS,)),
            pltpu.SemaphoreType.DMA((SENDS,)),
            pltpu.SemaphoreType.DMA((8,)),
            pltpu.SemaphoreType.DMA((28,)),
        ],
        compiler_params=pltpu.CompilerParams(
            collective_id=0, has_side_effects=True, vmem_limit_bytes=67043328
        ),
    )(tokens, grad_out, gates, ids, w_gate, w_up, w_down, s_gate, s_up, s_down)


def solution(mesh):
    flat = P(("node", "local"), None)
    routed = P("node", None, "local")
    shared = P(None, "local")
    return jax.shard_map(
        expert_layer,
        mesh=mesh,
        in_specs=(flat,) * 4 + (routed,) * 3 + (shared,) * 3,
        out_specs=(flat, flat) + (routed,) * 3 + (P("node", "local"),) * 3,
        check_vma=False,
    )
```

```python
import jax
import jax.numpy as jnp
from jax import lax
from jax.experimental import pallas as pl
from jax.experimental.pallas import tpu as pltpu
from jax.sharding import PartitionSpec as P

MESH = pl.DeviceIdType.MESH
F32 = jnp.float32
BF16 = jnp.bfloat16
UNIT = 128
ROWS = 16
RING = 4


def dot(a, b, ca, cb):
    return lax.dot_general(a, b, (((ca,), (cb,)), ((), ())), preferred_element_type=F32)


def body(
    tok_ref, grad_ref, gate_ref, id_ref, wg_ref, wu_ref, wd_ref, sg_ref, su_ref, sd_ref,
    dx_ref, dgate_ref, dwg_ref, dwu_ref, dwd_ref, dsg_ref, dsu_ref, dsd_ref,
    given, outgo, income, relay, answer, reply, relay_back, tt, tg, xx, w_all, v_all, gg, acc_p, acc_u,
    r1, r2, q1, q2, sw, pw, z1, z2, dw, ds,
    send_sem, recv_sem, load_sem, store_sem,
):
    width = wg_ref.shape[1]
    wide = width + UNIT
    block = width // 8
    half_block = block // 2
    node, here = lax.axis_index("node"), lax.axis_index("local")
    z, core = node // 2, node % 2
    y, x = here // RING, here % RING

    def step(v, by):
        return (v + by) % RING

    x_plus, x_minus = (node, y * RING + step(x, 1)), (node, y * RING + step(x, 3))
    y_plus, y_minus = (node, step(y, 1) * RING + x), (node, step(y, 3) * RING + x)
    z_plus, z_minus = (step(z, 1) * 2 + core, here), (step(z, 3) * 2 + core, here)
    partner = (z * 2 + (1 - core), here)
    z_plus_other = (step(z, 1) * 2 + (1 - core), here)
    z_minus_other = (step(z, 3) * 2 + (1 - core), here)
    first = ((x_plus, x_minus), (y_plus, y_minus))
    second = ((y_plus, y_minus), (x_plus, x_minus))

    loads = []

    def load(src, dst):
        copy = pltpu.make_async_copy(src, dst, load_sem.at[len(loads)])
        copy.start()
        loads.append(copy)

    load(tok_ref, given.at[0])
    load(grad_ref, given.at[1])
    for i, ref in enumerate((wg_ref.at[0], wu_ref.at[0], sg_ref, su_ref)):
        load(ref, w_all.at[:, pl.ds(i * UNIT, UNIT)])
    for i, ref in enumerate((wd_ref.at[0], sd_ref)):
        load(ref, v_all.at[:, pl.ds(i * UNIT, UNIT)])

    barrier = pltpu.get_barrier_semaphore()
    for device in (
        x_plus, x_minus, y_plus, y_minus, z_plus, z_minus, z_plus_other, z_minus_other, partner
    ):
        pl.semaphore_signal(barrier, inc=1, device_id=device, device_id_type=MESH)

    count = ROWS
    slot_row = lax.broadcasted_iota(jnp.int32, (2 * ROWS, count), 0)
    slot_node = ((z + (slot_row >> 3)) & 3) * 2 + ((core + (slot_row >> 2)) & 1)
    ids = id_ref[...].astype(F32)
    gates = gate_ref[...].astype(F32)
    id_rows = [ids[k : k + 1] for k in range(3)]
    gate_rows = [gates[k : k + 1] for k in range(3)]
    names = [
        [(id_rows[k] == (2 * slot_node + e).astype(F32)).astype(F32) for k in range(3)]
        for e in range(2)
    ]
    named = [names[e][0] + names[e][1] + names[e][2] for e in range(2)]
    member = jnp.maximum(named[0], named[1])
    earlier = (
        lax.broadcasted_iota(jnp.int32, (count, count), 0)
        < lax.broadcasted_iota(jnp.int32, (count, count), 1)
    ).astype(BF16)
    ranking = dot(member.astype(BF16), earlier, 1, 0)
    pick = jnp.where(ranking == (slot_row & 3).astype(F32), member, 0.0)
    pick_bf16 = pick.astype(BF16)
    side = [
        jnp.sum(pick * sum(names[e][k] * gate_rows[k] for k in range(3)), axis=1, keepdims=True)
        for e in range(2)
    ]
    side.append(jnp.sum(pick * named[0] * named[1], axis=1, keepdims=True))
    slot_lane = lax.broadcasted_iota(jnp.int32, (2 * ROWS, UNIT), 1)
    columns = sum(jnp.where(slot_lane == i, side[i], 0.0) for i in range(3)).astype(BF16)
    for s in range(8):
        outgo[s, :, width:wide] = columns[4 * s : 4 * s + 4]
    for copy in loads[:2]:
        copy.wait()
    stretch = width // 7

    def cut_rows(k, carry):
        at = pl.multiple_of(k * stretch, UNIT)
        for i, offset in enumerate((0, wide)):
            value = dot(pick_bf16, given[i, :, pl.ds(at, stretch)], 1, 0)
            for s in range(8):
                outgo[s, :, pl.ds(pl.multiple_of(at + offset, UNIT), stretch)] = value[
                    4 * s : 4 * s + 4
                ].astype(BF16)
        return carry

    lax.fori_loop(0, 7, cut_rows, 0)
    pl.semaphore_wait(barrier, 9)

    sends = []

    def send(src, dst, device):
        copy = pltpu.make_async_remote_copy(
            src_ref=src, dst_ref=dst, send_sem=send_sem.at[len(sends)],
            recv_sem=recv_sem.at[len(sends)], device_id=device, device_id_type=MESH,
        )
        copy.start()
        sends.append(copy)
        return copy

    across = {
        (0, 1): send(outgo.at[1], income.at[1], partner),
        (3, 0): send(outgo.at[6], income.at[2], z_minus),
        (2, 0): send(outgo.at[4], relay.at[0], z_plus),
        (3, 1): send(outgo.at[7], income.at[3], z_minus_other),
        (1, 0): send(outgo.at[2], income.at[6], z_plus),
        (2, 1): send(outgo.at[5], relay.at[1], z_minus),
        (1, 1): send(outgo.at[3], income.at[7], z_plus_other),
    }

    def stack(h):
        def piece(at, size):
            return jnp.concatenate(
                [
                    (outgo if h == 0 and s == 0 else income)[4 * h + s, :, pl.ds(at, size)].astype(F32)
                    for s in range(4)
                ],
                0,
            ).astype(BF16)

        def one_stretch(k, carry):
            at = pl.multiple_of(k * stretch, UNIT)
            tt[h, 0, 0, :, pl.ds(at, stretch)] = piece(at, stretch)
            tg[h, 0, 0, :, pl.ds(at, stretch)] = piece(pl.multiple_of(at + wide, UNIT), stretch)
            return carry

        lax.fori_loop(0, 7, one_stretch, 0)
        tt[h, 0, 0, :, width:] = piece(width, UNIT)

    one, two, far = {}, {}, {}

    def first_hop(h):
        plus, minus = first[h]
        for part, (a, b) in enumerate(((tt, tg), (tg, tt))):
            one[h, "p", part] = send(a.at[h, 0, 0], a.at[h, 0, 3], plus)
            one[h, "m", part] = send(b.at[h, 0, 0], b.at[h, 0, 1], minus)

    across[2, 0].wait_recv()
    forth = [send(relay.at[0], income.at[4], z_plus)]
    for key in ((0, 1), (3, 0), (3, 1)):
        across[key].wait_recv()
    stack(0)
    first_hop(0)
    across[2, 1].wait_recv()
    forth.append(send(relay.at[1], income.at[5], z_minus_other))

    def second_hop(h, d):
        plus, minus = second[h]
        two[h, d, "pt"] = send(tt.at[h, 0, d], tt.at[h, 3, d], plus)
        two[h, d, "mg"] = send(tg.at[h, 0, d], tg.at[h, 1, d], minus)
        two[h, d, "pg"] = send(tg.at[h, 0, d], tg.at[h, 3, d], plus)
        two[h, d, "mt"] = send(tt.at[h, 0, d], tt.at[h, 1, d], minus)

    def pass_on(h):
        plus, minus = first[h]
        one[h, "p", 0].wait_recv()
        far[h, "p"] = send(tt.at[h, 0, 3], tt.at[h, 0, 2], plus)
        one[h, "m", 0].wait_recv()
        far[h, "m"] = send(tg.at[h, 0, 1], tg.at[h, 0, 2], minus)

    second_hop(0, 0)
    for copy in (across[1, 0], across[1, 1], *forth):
        copy.wait_recv()
    stack(1)
    first_hop(1)
    pass_on(0)
    second_hop(1, 0)
    pass_on(1)
    for h in range(2):
        one[h, "p", 1].wait_recv()
        second_hop(h, 3)
    for h in range(2):
        one[h, "m", 1].wait_recv()
        second_hop(h, 1)
    for h in range(2):
        far[h, "p"].wait_recv()
        far[h, "m"].wait_recv()
        second_hop(h, 2)

    rows = 2 * RING * ROWS
    expert = here // (RING * RING // 2)
    lane = lax.broadcasted_iota(jnp.int32, (RING * ROWS, UNIT), 1)
    depth = width // 7

    def compute(i):
        acc_p[...] = jnp.zeros_like(acc_p)
        acc_u[...] = jnp.zeros_like(acc_u)

        def forward(k, carry):
            at = pl.ds(pl.multiple_of(k * depth, UNIT), depth)
            t = jnp.concatenate([tt[h, i, :, :, at].reshape(rows // 2, depth) for h in range(2)], 0)
            g = jnp.concatenate([tg[h, i, :, :, at].reshape(rows // 2, depth) for h in range(2)], 0)
            acc_p[...] += dot(t, w_all[at, :], 1, 0)
            acc_u[...] += dot(g, v_all[at, :], 1, 0)
            return carry

        lax.fori_loop(0, 7, forward, 0)
        for h in range(2):
            mine = slice(h * rows // 2, (h + 1) * rows // 2)
            side = tt[h, i, :, :, width:].reshape(rows // 2, UNIT).astype(F32)
            gate = jnp.where(expert == 0, side[:, 0:1], side[:, 1:2])
            for j, weight in enumerate((gate, side[:, 2:3])):
                pre = acc_p[mine, 2 * j * UNIT : (2 * j + 1) * UNIT]
                up = acc_p[mine, (2 * j + 1) * UNIT : (2 * j + 2) * UNIT]
                upstream = acc_u[mine, j * UNIT : (j + 1) * UNIT]
                sig = 1.0 / (1.0 + jnp.exp(-pre))
                activ = pre * sig
                slope = sig * (1.0 + pre * (1.0 - sig))
                hidden = activ * up
                scaled = weight * upstream
                for place, value in (
                    (2 * j, scaled * up * slope),
                    (2 * j + 1, scaled * activ),
                    (4 + j, weight * hidden),
                ):
                    gg[h, i, :, :, place * UNIT : (place + 1) * UNIT] = value.astype(BF16).reshape(
                        RING, ROWS, UNIT
                    )
                if j == 0:
                    score = jnp.sum(hidden * upstream, axis=1, keepdims=True)
                    xx[h, i, :, :, width:] = (
                        jnp.where(lane == expert, score, 0.0).astype(BF16).reshape(RING, ROWS, UNIT)
                    )

        def backward(k, carry):
            at = pl.ds(pl.multiple_of(k * (depth // 2), UNIT), depth // 2)
            g = jnp.concatenate(
                [gg[h, i, :, :, : 4 * UNIT].reshape(rows // 2, 4 * UNIT) for h in range(2)], 0
            )
            value = dot(g, w_all[at, :], 1, 1).astype(BF16)
            for h in range(2):
                xx[h, i, :, :, at] = value[h * rows // 2 : (h + 1) * rows // 2].reshape(
                    RING, ROWS, depth // 2
                )
            return carry

        lax.fori_loop(0, 14, backward, 0)

    for copy in loads[2:]:
        copy.wait()
    compute(0)
    onward = {}
    for d in (0, 3, 1, 2):
        for h in range(2):
            plus, minus = second[h]
            two[h, d, "pt"].wait_recv()
            onward[h, d, "p"] = send(tt.at[h, 3, d], tt.at[h, 2, d], plus)
            two[h, d, "mg"].wait_recv()
            onward[h, d, "m"] = send(tg.at[h, 1, d], tg.at[h, 2, d], minus)
    for d in range(RING):
        for h in range(2):
            two[h, d, "pg"].wait_recv()
            two[h, d, "mt"].wait_recv()
    compute(1)
    compute(3)
    upper, lower = (2, 1), (3, 0)
    full = {}
    for h in range(2):
        plus, minus = second[h]
        for j in range(2):
            full[h, "p", lower[j]] = send(xx.at[h, 1, lower[j]], r2.at[h, 0, lower[j]], plus)
            full[h, "m", upper[j]] = send(xx.at[h, 3, upper[j]], r2.at[h, 1, upper[j]], minus)
    for copy in onward.values():
        copy.wait_recv()
    compute(2)
    back = {}
    for j in range(2):
        for h in range(2):
            plus, minus = second[h]
            back[h, "p", j] = send(xx.at[h, 2, upper[j]], r1.at[h, 0, j], plus)
            back[h, "m", j] = send(xx.at[h, 2, lower[j]], r1.at[h, 1, j], minus)

    stores = []

    def store(src, dst):
        copy = pltpu.make_async_copy(src, dst, store_sem.at[len(stores)])
        copy.start()
        stores.append(copy)

    everything = 2 * RING * RING * ROWS

    def weights(parity):
        def one_block(k, carry):
            b = 2 * k + parity
            at = pl.ds(pl.multiple_of(b * block, UNIT), block)
            t = tt[:, :, :, :, at].reshape(everything, block)
            g = tg[:, :, :, :, at].reshape(everything, block)
            a = dot(t, gg[:, :, :, :, : 4 * UNIT].reshape(everything, 4 * UNIT), 0, 0)
            c = dot(g, gg[:, :, :, :, 4 * UNIT :].reshape(everything, 2 * UNIT), 0, 0)
            dw[0, b] = a[:, :UNIT].astype(BF16)
            dw[1, b] = a[:, UNIT : 2 * UNIT].astype(BF16)
            dw[2, b] = c[:, :UNIT].astype(BF16)
            sw[parity, k, :, : 2 * UNIT] = a[:, 2 * UNIT :].astype(BF16)
            sw[parity, k, :, 2 * UNIT :] = c[:, UNIT:].astype(BF16)
            return carry

        lax.fori_loop(0, RING, one_block, 0)

    def add(dst, *srcs):
        total = dst[...].astype(F32)
        for src in srcs:
            total = total + src[...].astype(F32)
        dst[...] = total.astype(BF16)

    weights(1 - core)
    swap = send(sw.at[1 - core], pw, partner)
    for j in range(2):
        for h in range(2):
            plus, minus = second[h]
            back[h, "p", j].wait_recv()
            add(xx.at[h, 1, upper[j]], r1.at[h, 0, j])
            full[h, "p", upper[j]] = send(xx.at[h, 1, upper[j]], r2.at[h, 0, upper[j]], plus)
            back[h, "m", j].wait_recv()
            add(xx.at[h, 3, lower[j]], r1.at[h, 1, j])
            full[h, "m", lower[j]] = send(xx.at[h, 3, lower[j]], r2.at[h, 1, lower[j]], minus)
    weights(core)
    for b in range(8):
        for j, ref in enumerate((dwg_ref, dwu_ref, dwd_ref)):
            store(dw.at[j, b], ref.at[0, pl.ds(b * block, block)])
    swap.wait_recv()

    def add_swap(k, carry):
        add(sw.at[core, k], pw.at[k])
        return carry

    lax.fori_loop(0, RING, add_swap, 0)
    low, high = pl.ds(0, half_block), pl.ds(half_block, half_block)
    z_back = (
        send(sw.at[core, step(z, 2), low], z1.at[0], z_plus),
        send(sw.at[core, step(z, 2), high], z1.at[1], z_minus),
    )
    z_full = [
        send(sw.at[core, step(z, 1), high], z2.at[0, high], z_plus),
        send(sw.at[core, step(z, 3), low], z2.at[1, low], z_minus),
    ]

    cut = (wide // UNIT + 1) // 2 * UNIT
    left, right = pl.ds(0, cut), pl.ds(cut, wide - cut)
    for d in (2, 3, 1, 0):
        for h in range(2):
            full[h, "p", d].wait_recv()
            full[h, "m", d].wait_recv()
            add(xx.at[h, 0, d], r2.at[h, 0, d], r2.at[h, 1, d])
            plus, minus = first[h]
            if d == 2:
                back[h, "P"] = send(xx.at[h, 0, 2, :, left], q1.at[h, 0, :, left], plus)
                back[h, "M"] = send(xx.at[h, 0, 2, :, right], q1.at[h, 1, :, right], minus)
            if d == 1:
                full[h, "P"] = send(xx.at[h, 0, 1, :, right], q2.at[h, 0, :, right], plus)
            if d == 3:
                full[h, "M"] = send(xx.at[h, 0, 3, :, left], q2.at[h, 1, :, left], minus)
    z_back[0].wait_recv()
    add(sw.at[core, step(z, 1), low], z1.at[0])
    z_full.append(send(sw.at[core, step(z, 1), low], z2.at[0, low], z_plus))
    z_back[1].wait_recv()
    add(sw.at[core, step(z, 3), high], z1.at[1])
    z_full.append(send(sw.at[core, step(z, 3), high], z2.at[1, high], z_minus))
    last = []
    for h in range(2):
        plus, minus = first[h]
        back[h, "P"].wait_recv()
        add(xx.at[h, 0, 1, :, left], q1.at[h, 0, :, left])
        last.append(send(xx.at[h, 0, 1, :, left], q2.at[h, 0, :, left], plus))
        back[h, "M"].wait_recv()
        add(xx.at[h, 0, 3, :, right], q1.at[h, 1, :, right])
        last.append(send(xx.at[h, 0, 3, :, right], q2.at[h, 1, :, right], minus))
    for h in range(2):
        full[h, "P"].wait_recv()
        full[h, "M"].wait_recv()
        last[2 * h].wait_recv()
        last[2 * h + 1].wait_recv()

        def one_stretch(k, carry, h=h):
            at = pl.ds(pl.multiple_of(k * 3 * UNIT, UNIT), 3 * UNIT)
            total = xx[h, 0, 0, :, at].astype(F32)
            for i in range(2):
                total = total + q2[h, i, :, at].astype(F32)
            for s in range(4):
                answer[4 * h + s, :, at] = total[4 * s : 4 * s + 4].astype(BF16)
            return carry

        lax.fori_loop(0, wide // (3 * UNIT), one_stretch, 0)
        if h == 0:
            home = [
                send(answer.at[2], reply.at[6], z_plus),
                send(answer.at[3], reply.at[7], z_plus_other),
                send(answer.at[1], reply.at[1], partner),
            ]
        else:
            home += [
                send(answer.at[4], relay_back.at[0], z_plus),
                send(answer.at[5], relay_back.at[1], z_minus),
                send(answer.at[6], reply.at[2], z_minus),
                send(answer.at[7], reply.at[3], z_minus_other),
            ]
    for copy in z_full:
        copy.wait_recv()
    total = sw[core, z].astype(F32) + z2[0].astype(F32) + z2[1].astype(F32)
    for j, ref in enumerate((dsg_ref, dsu_ref, dsd_ref)):
        ds[j] = total[:, j * UNIT : (j + 1) * UNIT].astype(BF16)
        store(ds.at[j], ref)
    home[3].wait_recv()
    home.append(send(relay_back.at[0], reply.at[4], z_plus))
    home[4].wait_recv()
    home.append(send(relay_back.at[1], reply.at[5], z_minus_other))
    for i in (0, 1, 2, 5, 6, 7, 8):
        home[i].wait_recv()

    def answers(at, size):
        return jnp.concatenate(
            [(answer if s == 0 else reply)[s, :, pl.ds(at, size)].astype(F32) for s in range(8)], 0
        )

    def finish(k, carry):
        at = pl.multiple_of(k * stretch, UNIT)
        total = dot(pick_bf16, answers(at, stretch).astype(BF16), 0, 0)
        given[0, :, pl.ds(at, stretch)] = total.astype(BF16)
        return carry

    lax.fori_loop(0, 7, finish, 0)
    store(given.at[0], dx_ref)
    score = answers(width, UNIT)
    for k in range(3):
        dgate_ref[k : k + 1] = jnp.sum(
            pick * (names[0][k] * score[:, 0:1] + names[1][k] * score[:, 1:2]),
            axis=0, keepdims=True,
        )
    for copy in sends:
        copy.wait_send()
    for copy in stores:
        copy.wait()


PIECES = 8


def hand_on(*refs):
    ins, outs, held, sems = refs[:8], refs[8:16], refs[16:24], refs[24]
    copies = []
    for i in (1, 2, 3, 4, 5, 6, 0, 7):
        for p in range(PIECES if 1 <= i <= 3 else 1):
            at = pl.ds(p * (held[i].shape[1] // PIECES), held[i].shape[1] // PIECES)
            view = (lambda r, at=at: r.at[0, at]) if 1 <= i <= 3 else (lambda r: r)
            pair = [
                pltpu.make_async_copy(view(src), view(dst), sems.at[j, i * PIECES + p])
                for j, (src, dst) in enumerate(((ins[i], held[i]), (held[i], outs[i])))
            ]
            pair[0].start()
            copies.append(pair)
    for pair in copies:
        pair[0].wait()
        pair[1].start()
    for pair in copies:
        pair[1].wait()


SENDS = 103 + 9 + 9


def expert_layer(tokens, grad_out, gates, ids, w_gate, w_up, w_down, s_gate, s_up, s_down):
    width = s_gate.shape[0]
    wide = width + UNIT
    block = width // 8
    shape = jax.ShapeDtypeStruct
    anywhere = pl.BlockSpec(memory_space=pl.ANY)
    inside = pl.BlockSpec(memory_space=pltpu.VMEM)
    dx, dgates, *grads = pl.pallas_call(
        body,
        out_shape=(
            shape(tokens.shape, BF16),
            shape(gates.shape[::-1], F32),
            *(shape(w_gate.shape, BF16) for _ in range(3)),
            *(shape((block, UNIT), BF16) for _ in range(3)),
        ),
        in_specs=[anywhere] * 2 + [inside] * 2 + [anywhere] * 6,
        out_specs=(anywhere, inside) + (anywhere,) * 6,
        scratch_shapes=[
            pltpu.VMEM((2, ROWS, width), BF16),
            pltpu.VMEM((8, 4, wide + width), BF16),
            pltpu.VMEM((8, 4, wide + width), BF16),
            pltpu.VMEM((2, 4, wide + width), BF16),
            pltpu.VMEM((8, 4, wide), BF16),
            pltpu.VMEM((8, 4, wide), BF16),
            pltpu.VMEM((2, 4, wide), BF16),
            pltpu.VMEM((2, RING, RING, ROWS, wide), BF16),
            pltpu.VMEM((2, RING, RING, ROWS, width), BF16),
            pltpu.VMEM((2, RING, RING, ROWS, wide), BF16),
            pltpu.VMEM((width, 4 * UNIT), BF16),
            pltpu.VMEM((width, 2 * UNIT), BF16),
            pltpu.VMEM((2, RING, RING, ROWS, 6 * UNIT), BF16),
            pltpu.VMEM((2 * RING * ROWS, 4 * UNIT), F32),
            pltpu.VMEM((2 * RING * ROWS, 2 * UNIT), F32),
            pltpu.VMEM((2, 2, 2, ROWS, wide), BF16),
            pltpu.VMEM((2, 2, RING, ROWS, wide), BF16),
            pltpu.VMEM((2, 2, ROWS, wide), BF16),
            pltpu.VMEM((2, 2, ROWS, wide), BF16),
            pltpu.VMEM((2, RING, block, 3 * UNIT), BF16),
            pltpu.VMEM((RING, block, 3 * UNIT), BF16),
            pltpu.VMEM((2, block // 2, 3 * UNIT), BF16),
            pltpu.VMEM((2, block, 3 * UNIT), BF16),
            pltpu.VMEM((3, 8, block, UNIT), BF16),
            pltpu.VMEM((3, block, UNIT), BF16),
            pltpu.SemaphoreType.DMA((SENDS,)),
            pltpu.SemaphoreType.DMA((SENDS,)),
            pltpu.SemaphoreType.DMA((8,)),
            pltpu.SemaphoreType.DMA((28,)),
        ],
        compiler_params=pltpu.CompilerParams(
            collective_id=0, has_side_effects=True, vmem_limit_bytes=67043328
        ),
    )(tokens, grad_out, gates.T, ids.T, w_gate, w_up, w_down, s_gate, s_up, s_down)
    outs = (dx, *grads, dgates)
    dx, *grads, dgates = pl.pallas_call(
        hand_on,
        out_shape=tuple(shape(o.shape, o.dtype) for o in outs),
        in_specs=[anywhere] * 8,
        out_specs=(anywhere,) * 8,
        scratch_shapes=[
            *(pltpu.VMEM(o.shape, o.dtype) for o in outs),
            pltpu.SemaphoreType.DMA((2, 8 * PIECES)),
        ],
        compiler_params=pltpu.CompilerParams(vmem_limit_bytes=67043328),
    )(*outs)
    return (dx, dgates.T, *grads)


def solution(mesh):
    flat = P(("node", "local"), None)
    routed = P("node", None, "local")
    shared = P(None, "local")
    return jax.shard_map(
        expert_layer,
        mesh=mesh,
        in_specs=(flat,) * 4 + (routed,) * 3 + (shared,) * 3,
        out_specs=(flat, flat) + (routed,) * 3 + (P("node", "local"),) * 3,
        check_vma=False,
    )
```

```python
import jax
import jax.numpy as jnp
from jax import lax
from jax.experimental import pallas as pl
from jax.experimental.pallas import tpu as pltpu
from jax.sharding import PartitionSpec as P

MESH = pl.DeviceIdType.MESH
F32 = jnp.float32
BF16 = jnp.bfloat16
UNIT = 128
ROWS = 16
RING = 4


def dot(a, b, ca, cb):
    return lax.dot_general(a, b, (((ca,), (cb,)), ((), ())), preferred_element_type=F32)


def body(
    tok_ref, grad_ref, gate_ref, id_ref, wg_ref, wu_ref, wd_ref, sg_ref, su_ref, sd_ref,
    dx_ref, dgate_ref, dwg_ref, dwu_ref, dwd_ref, dsg_ref, dsu_ref, dsd_ref,
    given, outgo, income, relay, answer, reply, relay_back, tt, tg, xx, w_all, v_all, gg, acc_p, acc_u,
    r1, r2, q1, q2, sw, pw, z1, z2,
    send_sem, recv_sem, load_sem,
):
    width = wg_ref.shape[1]
    wide = width + UNIT
    block = width // 8
    half_block = block // 2
    node, here = lax.axis_index("node"), lax.axis_index("local")
    z, core = node // 2, node % 2
    y, x = here // RING, here % RING

    def step(v, by):
        return (v + by) % RING

    x_plus, x_minus = (node, y * RING + step(x, 1)), (node, y * RING + step(x, 3))
    y_plus, y_minus = (node, step(y, 1) * RING + x), (node, step(y, 3) * RING + x)
    z_plus, z_minus = (step(z, 1) * 2 + core, here), (step(z, 3) * 2 + core, here)
    partner = (z * 2 + (1 - core), here)
    z_plus_other = (step(z, 1) * 2 + (1 - core), here)
    z_minus_other = (step(z, 3) * 2 + (1 - core), here)
    first = ((x_plus, x_minus), (y_plus, y_minus))
    second = ((y_plus, y_minus), (x_plus, x_minus))

    loads = []

    def load(src, dst):
        copy = pltpu.make_async_copy(src, dst, load_sem.at[len(loads)])
        copy.start()
        loads.append(copy)

    load(tok_ref, given.at[0])
    load(grad_ref, given.at[1])
    barrier = pltpu.get_barrier_semaphore()
    for device in (
        x_plus, x_minus, y_plus, y_minus, z_plus, z_minus, z_plus_other, z_minus_other, partner
    ):
        pl.semaphore_signal(barrier, inc=1, device_id=device, device_id_type=MESH)

    count = ROWS
    slot_row = lax.broadcasted_iota(jnp.int32, (2 * ROWS, count), 0)
    slot_node = ((z + (slot_row >> 3)) & 3) * 2 + ((core + (slot_row >> 2)) & 1)
    ids = id_ref[...].astype(F32)
    gates = gate_ref[...].astype(F32)
    id_rows = [ids[k : k + 1] for k in range(3)]
    gate_rows = [gates[k : k + 1] for k in range(3)]
    names = [
        [(id_rows[k] == (2 * slot_node + e).astype(F32)).astype(F32) for k in range(3)]
        for e in range(2)
    ]
    named = [names[e][0] + names[e][1] + names[e][2] for e in range(2)]
    member = jnp.maximum(named[0], named[1])
    earlier = (
        lax.broadcasted_iota(jnp.int32, (count, count), 0)
        < lax.broadcasted_iota(jnp.int32, (count, count), 1)
    ).astype(BF16)
    ranking = dot(member.astype(BF16), earlier, 1, 0)
    pick = jnp.where(ranking == (slot_row & 3).astype(F32), member, 0.0)
    pick_bf16 = pick.astype(BF16)
    side = [
        jnp.sum(pick * sum(names[e][k] * gate_rows[k] for k in range(3)), axis=1, keepdims=True)
        for e in range(2)
    ]
    side.append(jnp.sum(pick * named[0] * named[1], axis=1, keepdims=True))
    slot_lane = lax.broadcasted_iota(jnp.int32, (2 * ROWS, UNIT), 1)
    columns = sum(jnp.where(slot_lane == i, side[i], 0.0) for i in range(3)).astype(BF16)
    for s in range(8):
        outgo[s, :, width:wide] = columns[4 * s : 4 * s + 4]
    for copy in loads[:2]:
        copy.wait()
    stretch = width // 7

    def cut_rows(k, carry):
        at = pl.multiple_of(k * stretch, UNIT)
        for i, offset in enumerate((0, wide)):
            value = dot(pick_bf16, given[i, :, pl.ds(at, stretch)], 1, 0)
            for s in range(8):
                outgo[s, :, pl.ds(pl.multiple_of(at + offset, UNIT), stretch)] = value[
                    4 * s : 4 * s + 4
                ].astype(BF16)
        return carry

    lax.fori_loop(0, 7, cut_rows, 0)
    pl.semaphore_wait(barrier, 9)

    sends = []

    def send(src, dst, device):
        copy = pltpu.make_async_remote_copy(
            src_ref=src, dst_ref=dst, send_sem=send_sem.at[len(sends)],
            recv_sem=recv_sem.at[len(sends)], device_id=device, device_id_type=MESH,
        )
        copy.start()
        sends.append(copy)
        return copy

    across = {
        (0, 1): send(outgo.at[1], income.at[1], partner),
        (3, 0): send(outgo.at[6], income.at[2], z_minus),
        (2, 0): send(outgo.at[4], relay.at[0], z_plus),
        (3, 1): send(outgo.at[7], income.at[3], z_minus_other),
        (1, 0): send(outgo.at[2], income.at[6], z_plus),
        (2, 1): send(outgo.at[5], relay.at[1], z_minus),
        (1, 1): send(outgo.at[3], income.at[7], z_plus_other),
    }

    for i, ref in enumerate((wg_ref.at[0], wu_ref.at[0], sg_ref, su_ref)):
        load(ref, w_all.at[:, pl.ds(i * UNIT, UNIT)])
    for i, ref in enumerate((wd_ref.at[0], sd_ref)):
        load(ref, v_all.at[:, pl.ds(i * UNIT, UNIT)])

    def stack(h):
        def piece(at, size):
            return jnp.concatenate(
                [
                    (outgo if h == 0 and s == 0 else income)[4 * h + s, :, pl.ds(at, size)].astype(F32)
                    for s in range(4)
                ],
                0,
            ).astype(BF16)

        def one_stretch(k, carry):
            at = pl.multiple_of(k * stretch, UNIT)
            tt[h, 0, 0, :, pl.ds(at, stretch)] = piece(at, stretch)
            tg[h, 0, 0, :, pl.ds(at, stretch)] = piece(pl.multiple_of(at + wide, UNIT), stretch)
            return carry

        lax.fori_loop(0, 7, one_stretch, 0)
        tt[h, 0, 0, :, width:] = piece(width, UNIT)

    one, two, far = {}, {}, {}

    def first_hop(h):
        plus, minus = first[h]
        for part, (a, b) in enumerate(((tt, tg), (tg, tt))):
            one[h, "p", part] = send(a.at[h, 0, 0], a.at[h, 0, 3], plus)
            one[h, "m", part] = send(b.at[h, 0, 0], b.at[h, 0, 1], minus)

    across[2, 0].wait_recv()
    forth = [send(relay.at[0], income.at[4], z_plus)]
    for key in ((0, 1), (3, 0), (3, 1)):
        across[key].wait_recv()
    stack(0)
    first_hop(0)
    across[2, 1].wait_recv()
    forth.append(send(relay.at[1], income.at[5], z_minus_other))

    def second_hop(h, d):
        plus, minus = second[h]
        two[h, d, "pt"] = send(tt.at[h, 0, d], tt.at[h, 3, d], plus)
        two[h, d, "mg"] = send(tg.at[h, 0, d], tg.at[h, 1, d], minus)
        two[h, d, "pg"] = send(tg.at[h, 0, d], tg.at[h, 3, d], plus)
        two[h, d, "mt"] = send(tt.at[h, 0, d], tt.at[h, 1, d], minus)

    def pass_on(h):
        plus, minus = first[h]
        one[h, "p", 0].wait_recv()
        far[h, "p"] = send(tt.at[h, 0, 3], tt.at[h, 0, 2], plus)
        one[h, "m", 0].wait_recv()
        far[h, "m"] = send(tg.at[h, 0, 1], tg.at[h, 0, 2], minus)

    second_hop(0, 0)
    for copy in (across[1, 0], across[1, 1], *forth):
        copy.wait_recv()
    stack(1)
    first_hop(1)
    pass_on(0)
    second_hop(1, 0)
    pass_on(1)
    for h in range(2):
        one[h, "p", 1].wait_recv()
        second_hop(h, 3)
    for h in range(2):
        one[h, "m", 1].wait_recv()
        second_hop(h, 1)
    for h in range(2):
        far[h, "p"].wait_recv()
        far[h, "m"].wait_recv()
        second_hop(h, 2)

    rows = 2 * RING * ROWS
    expert = here // (RING * RING // 2)
    lane = lax.broadcasted_iota(jnp.int32, (RING * ROWS, UNIT), 1)
    depth = width // 7

    def compute(i):
        acc_p[...] = jnp.zeros_like(acc_p)
        acc_u[...] = jnp.zeros_like(acc_u)

        def forward(k, carry):
            at = pl.ds(pl.multiple_of(k * depth, UNIT), depth)
            t = jnp.concatenate([tt[h, i, :, :, at].reshape(rows // 2, depth) for h in range(2)], 0)
            g = jnp.concatenate([tg[h, i, :, :, at].reshape(rows // 2, depth) for h in range(2)], 0)
            acc_p[...] += dot(t, w_all[at, :], 1, 0)
            acc_u[...] += dot(g, v_all[at, :], 1, 0)
            return carry

        lax.fori_loop(0, 7, forward, 0)
        for h in range(2):
            mine = slice(h * rows // 2, (h + 1) * rows // 2)
            side = tt[h, i, :, :, width:].reshape(rows // 2, UNIT).astype(F32)
            gate = jnp.where(expert == 0, side[:, 0:1], side[:, 1:2])
            for j, weight in enumerate((gate, side[:, 2:3])):
                pre = acc_p[mine, 2 * j * UNIT : (2 * j + 1) * UNIT]
                up = acc_p[mine, (2 * j + 1) * UNIT : (2 * j + 2) * UNIT]
                upstream = acc_u[mine, j * UNIT : (j + 1) * UNIT]
                sig = 1.0 / (1.0 + jnp.exp(-pre))
                activ = pre * sig
                slope = sig * (1.0 + pre * (1.0 - sig))
                hidden = activ * up
                scaled = weight * upstream
                for place, value in (
                    (2 * j, scaled * up * slope),
                    (2 * j + 1, scaled * activ),
                    (4 + j, weight * hidden),
                ):
                    gg[h, i, :, :, place * UNIT : (place + 1) * UNIT] = value.astype(BF16).reshape(
                        RING, ROWS, UNIT
                    )
                if j == 0:
                    score = jnp.sum(hidden * upstream, axis=1, keepdims=True)
                    xx[h, i, :, :, width:] = (
                        jnp.where(lane == expert, score, 0.0).astype(BF16).reshape(RING, ROWS, UNIT)
                    )

        def backward(k, carry):
            at = pl.ds(pl.multiple_of(k * (depth // 2), UNIT), depth // 2)
            g = jnp.concatenate(
                [gg[h, i, :, :, : 4 * UNIT].reshape(rows // 2, 4 * UNIT) for h in range(2)], 0
            )
            value = dot(g, w_all[at, :], 1, 1).astype(BF16)
            for h in range(2):
                xx[h, i, :, :, at] = value[h * rows // 2 : (h + 1) * rows // 2].reshape(
                    RING, ROWS, depth // 2
                )
            return carry

        lax.fori_loop(0, 14, backward, 0)

    for copy in loads[2:]:
        copy.wait()
    compute(0)
    onward = {}
    for d in (0, 3, 1, 2):
        for h in range(2):
            plus, minus = second[h]
            two[h, d, "pt"].wait_recv()
            onward[h, d, "p"] = send(tt.at[h, 3, d], tt.at[h, 2, d], plus)
            two[h, d, "mg"].wait_recv()
            onward[h, d, "m"] = send(tg.at[h, 1, d], tg.at[h, 2, d], minus)
    for d in range(RING):
        for h in range(2):
            two[h, d, "pg"].wait_recv()
            two[h, d, "mt"].wait_recv()
    compute(1)
    compute(3)
    upper, lower = (2, 1), (3, 0)
    full = {}
    for h in range(2):
        plus, minus = second[h]
        for j in range(2):
            full[h, "p", lower[j]] = send(xx.at[h, 1, lower[j]], r2.at[h, 0, lower[j]], plus)
            full[h, "m", upper[j]] = send(xx.at[h, 3, upper[j]], r2.at[h, 1, upper[j]], minus)
    for copy in onward.values():
        copy.wait_recv()
    compute(2)
    back = {}
    for j in range(2):
        for h in range(2):
            plus, minus = second[h]
            back[h, "p", j] = send(xx.at[h, 2, upper[j]], r1.at[h, 0, j], plus)
            back[h, "m", j] = send(xx.at[h, 2, lower[j]], r1.at[h, 1, j], minus)

    everything = 2 * RING * RING * ROWS

    def weights(parity):
        def one_block(k, carry):
            b = 2 * k + parity
            at = pl.ds(pl.multiple_of(b * block, UNIT), block)
            t = tt[:, :, :, :, at].reshape(everything, block)
            g = tg[:, :, :, :, at].reshape(everything, block)
            a = dot(t, gg[:, :, :, :, : 4 * UNIT].reshape(everything, 4 * UNIT), 0, 0)
            c = dot(g, gg[:, :, :, :, 4 * UNIT :].reshape(everything, 2 * UNIT), 0, 0)
            dwg_ref[0, at] = a[:, :UNIT].astype(BF16)
            dwu_ref[0, at] = a[:, UNIT : 2 * UNIT].astype(BF16)
            dwd_ref[0, at] = c[:, :UNIT].astype(BF16)
            sw[parity, k, :, : 2 * UNIT] = a[:, 2 * UNIT :].astype(BF16)
            sw[parity, k, :, 2 * UNIT :] = c[:, UNIT:].astype(BF16)
            return carry

        lax.fori_loop(0, RING, one_block, 0)

    def add(dst, *srcs):
        total = dst[...].astype(F32)
        for src in srcs:
            total = total + src[...].astype(F32)
        dst[...] = total.astype(BF16)

    weights(1 - core)
    swap = send(sw.at[1 - core], pw, partner)
    for j in range(2):
        for h in range(2):
            plus, minus = second[h]
            back[h, "p", j].wait_recv()
            add(xx.at[h, 1, upper[j]], r1.at[h, 0, j])
            full[h, "p", upper[j]] = send(xx.at[h, 1, upper[j]], r2.at[h, 0, upper[j]], plus)
            back[h, "m", j].wait_recv()
            add(xx.at[h, 3, lower[j]], r1.at[h, 1, j])
            full[h, "m", lower[j]] = send(xx.at[h, 3, lower[j]], r2.at[h, 1, lower[j]], minus)
    weights(core)
    swap.wait_recv()

    def add_swap(k, carry):
        add(sw.at[core, k], pw.at[k])
        return carry

    lax.fori_loop(0, RING, add_swap, 0)
    low, high = pl.ds(0, half_block), pl.ds(half_block, half_block)
    z_back = (
        send(sw.at[core, step(z, 2), low], z1.at[0], z_plus),
        send(sw.at[core, step(z, 2), high], z1.at[1], z_minus),
    )
    z_full = [
        send(sw.at[core, step(z, 1), high], z2.at[0, high], z_plus),
        send(sw.at[core, step(z, 3), low], z2.at[1, low], z_minus),
    ]

    cut = (wide // UNIT + 1) // 2 * UNIT
    left, right = pl.ds(0, cut), pl.ds(cut, wide - cut)
    for d in (2, 3, 1, 0):
        for h in range(2):
            full[h, "p", d].wait_recv()
            full[h, "m", d].wait_recv()
            add(xx.at[h, 0, d], r2.at[h, 0, d], r2.at[h, 1, d])
            plus, minus = first[h]
            if d == 2:
                back[h, "P"] = send(xx.at[h, 0, 2, :, left], q1.at[h, 0, :, left], plus)
                back[h, "M"] = send(xx.at[h, 0, 2, :, right], q1.at[h, 1, :, right], minus)
            if d == 1:
                full[h, "P"] = send(xx.at[h, 0, 1, :, right], q2.at[h, 0, :, right], plus)
            if d == 3:
                full[h, "M"] = send(xx.at[h, 0, 3, :, left], q2.at[h, 1, :, left], minus)
    z_back[0].wait_recv()
    add(sw.at[core, step(z, 1), low], z1.at[0])
    z_full.append(send(sw.at[core, step(z, 1), low], z2.at[0, low], z_plus))
    z_back[1].wait_recv()
    add(sw.at[core, step(z, 3), high], z1.at[1])
    z_full.append(send(sw.at[core, step(z, 3), high], z2.at[1, high], z_minus))
    last = []
    for h in range(2):
        plus, minus = first[h]
        back[h, "P"].wait_recv()
        add(xx.at[h, 0, 1, :, left], q1.at[h, 0, :, left])
        last.append(send(xx.at[h, 0, 1, :, left], q2.at[h, 0, :, left], plus))
        back[h, "M"].wait_recv()
        add(xx.at[h, 0, 3, :, right], q1.at[h, 1, :, right])
        last.append(send(xx.at[h, 0, 3, :, right], q2.at[h, 1, :, right], minus))
    for h in range(2):
        full[h, "P"].wait_recv()
        full[h, "M"].wait_recv()
        last[2 * h].wait_recv()
        last[2 * h + 1].wait_recv()

        def one_stretch(k, carry, h=h):
            at = pl.ds(pl.multiple_of(k * 3 * UNIT, UNIT), 3 * UNIT)
            total = xx[h, 0, 0, :, at].astype(F32)
            for i in range(2):
                total = total + q2[h, i, :, at].astype(F32)
            for s in range(4):
                answer[4 * h + s, :, at] = total[4 * s : 4 * s + 4].astype(BF16)
            return carry

        lax.fori_loop(0, wide // (3 * UNIT), one_stretch, 0)
        if h == 0:
            home = [
                send(answer.at[2], reply.at[6], z_plus),
                send(answer.at[3], reply.at[7], z_plus_other),
                send(answer.at[1], reply.at[1], partner),
            ]
        else:
            home += [
                send(answer.at[4], relay_back.at[0], z_plus),
                send(answer.at[5], relay_back.at[1], z_minus),
                send(answer.at[6], reply.at[2], z_minus),
                send(answer.at[7], reply.at[3], z_minus_other),
            ]
    for copy in z_full:
        copy.wait_recv()
    total = sw[core, z].astype(F32) + z2[0].astype(F32) + z2[1].astype(F32)
    for j, ref in enumerate((dsg_ref, dsu_ref, dsd_ref)):
        ref[...] = total[:, j * UNIT : (j + 1) * UNIT].astype(BF16)
    home[3].wait_recv()
    home.append(send(relay_back.at[0], reply.at[4], z_plus))
    home[4].wait_recv()
    home.append(send(relay_back.at[1], reply.at[5], z_minus_other))
    for i in (0, 1, 2, 5, 6, 7, 8):
        home[i].wait_recv()

    def answers(at, size):
        return jnp.concatenate(
            [(answer if s == 0 else reply)[s, :, pl.ds(at, size)].astype(F32) for s in range(8)], 0
        )

    def finish(k, carry):
        at = pl.multiple_of(k * stretch, UNIT)
        total = dot(pick_bf16, answers(at, stretch).astype(BF16), 0, 0)
        dx_ref[:, pl.ds(at, stretch)] = total.astype(BF16)
        return carry

    lax.fori_loop(0, 7, finish, 0)
    score = answers(width, UNIT)
    for k in range(3):
        dgate_ref[k : k + 1] = jnp.sum(
            pick * (names[0][k] * score[:, 0:1] + names[1][k] * score[:, 1:2]),
            axis=0, keepdims=True,
        )
    for copy in sends:
        copy.wait_send()


def hand_on(*refs):
    ins, outs, sems = refs[:8], refs[8:16], refs[16]
    copies = [pltpu.make_async_copy(*pair, sems.at[i]) for i, pair in enumerate(zip(ins, outs))]
    for copy in copies:
        copy.start()
    for copy in copies:
        copy.wait()


SENDS = 103 + 9 + 9


def expert_layer(tokens, grad_out, gates, ids, w_gate, w_up, w_down, s_gate, s_up, s_down):
    width = s_gate.shape[0]
    wide = width + UNIT
    block = width // 8
    shape = jax.ShapeDtypeStruct
    anywhere = pl.BlockSpec(memory_space=pl.ANY)
    inside = pl.BlockSpec(memory_space=pltpu.VMEM)
    dx, dgates, *grads = pl.pallas_call(
        body,
        out_shape=(
            pltpu.VMEM(tokens.shape, BF16),
            pltpu.VMEM(gates.shape[::-1], F32),
            *(pltpu.VMEM(w_gate.shape, BF16) for _ in range(3)),
            *(pltpu.VMEM((block, UNIT), BF16) for _ in range(3)),
        ),
        in_specs=[anywhere] * 2 + [inside] * 2 + [anywhere] * 6,
        out_specs=(inside,) * 8,
        scratch_shapes=[
            pltpu.VMEM((2, ROWS, width), BF16),
            pltpu.VMEM((8, 4, wide + width), BF16),
            pltpu.VMEM((8, 4, wide + width), BF16),
            pltpu.VMEM((2, 4, wide + width), BF16),
            pltpu.VMEM((8, 4, wide), BF16),
            pltpu.VMEM((8, 4, wide), BF16),
            pltpu.VMEM((2, 4, wide), BF16),
            pltpu.VMEM((2, RING, RING, ROWS, wide), BF16),
            pltpu.VMEM((2, RING, RING, ROWS, width), BF16),
            pltpu.VMEM((2, RING, RING, ROWS, wide), BF16),
            pltpu.VMEM((width, 4 * UNIT), BF16),
            pltpu.VMEM((width, 2 * UNIT), BF16),
            pltpu.VMEM((2, RING, RING, ROWS, 6 * UNIT), BF16),
            pltpu.VMEM((2 * RING * ROWS, 4 * UNIT), F32),
            pltpu.VMEM((2 * RING * ROWS, 2 * UNIT), F32),
            pltpu.VMEM((2, 2, 2, ROWS, wide), BF16),
            pltpu.VMEM((2, 2, RING, ROWS, wide), BF16),
            pltpu.VMEM((2, 2, ROWS, wide), BF16),
            pltpu.VMEM((2, 2, ROWS, wide), BF16),
            pltpu.VMEM((2, RING, block, 3 * UNIT), BF16),
            pltpu.VMEM((RING, block, 3 * UNIT), BF16),
            pltpu.VMEM((2, block // 2, 3 * UNIT), BF16),
            pltpu.VMEM((2, block, 3 * UNIT), BF16),
            pltpu.SemaphoreType.DMA((SENDS,)),
            pltpu.SemaphoreType.DMA((SENDS,)),
            pltpu.SemaphoreType.DMA((8,)),
        ],
        compiler_params=pltpu.CompilerParams(
            collective_id=0, has_side_effects=True, vmem_limit_bytes=60500000
        ),
    )(tokens, grad_out, gates.T, ids.T, w_gate, w_up, w_down, s_gate, s_up, s_down)
    outs = (dx, *grads, dgates)
    dx, *grads, dgates = pl.pallas_call(
        hand_on,
        out_shape=tuple(shape(o.shape, o.dtype) for o in outs),
        in_specs=[inside] * 8,
        out_specs=(anywhere,) * 8,
        scratch_shapes=[pltpu.SemaphoreType.DMA((8,))],
        compiler_params=pltpu.CompilerParams(vmem_limit_bytes=8 * 2**20),
    )(*outs)
    return (dx, dgates.T, *grads)


def solution(mesh):
    flat = P(("node", "local"), None)
    routed = P("node", None, "local")
    shared = P(None, "local")
    return jax.shard_map(
        expert_layer,
        mesh=mesh,
        in_specs=(flat,) * 4 + (routed,) * 3 + (shared,) * 3,
        out_specs=(flat, flat) + (routed,) * 3 + (P("node", "local"),) * 3,
        check_vma=False,
    )
```

```python
import jax
import jax.numpy as jnp
from jax import lax
from jax.experimental import pallas as pl
from jax.experimental.pallas import tpu as pltpu
from jax.sharding import PartitionSpec as P

MESH = pl.DeviceIdType.MESH
F32 = jnp.float32
BF16 = jnp.bfloat16
UNIT = 128
ROWS = 16
RING = 4


def dot(a, b, ca, cb):
    return lax.dot_general(a, b, (((ca,), (cb,)), ((), ())), preferred_element_type=F32)


def body(
    tok_ref, grad_ref, gate_ref, id_ref, wg_ref, wu_ref, wd_ref, sg_ref, su_ref, sd_ref,
    dx_ref, dgate_ref, dwg_ref, dwu_ref, dwd_ref, dsg_ref, dsu_ref, dsd_ref,
    given, outgo, income, relay, answer, reply, relay_back, tt, tg, xx, w_all, v_all, gg, acc_p, acc_u,
    r1, r2, q1, q2, sw, pw, z1, z2,
    send_sem, recv_sem, load_sem,
):
    width = wg_ref.shape[1]
    wide = width + UNIT
    block = width // 8
    half_block = block // 2
    node, here = lax.axis_index("node"), lax.axis_index("local")
    z, core = node // 2, node % 2
    y, x = here // RING, here % RING

    def step(v, by):
        return (v + by) % RING

    x_plus, x_minus = (node, y * RING + step(x, 1)), (node, y * RING + step(x, 3))
    y_plus, y_minus = (node, step(y, 1) * RING + x), (node, step(y, 3) * RING + x)
    z_plus, z_minus = (step(z, 1) * 2 + core, here), (step(z, 3) * 2 + core, here)
    partner = (z * 2 + (1 - core), here)
    z_plus_other = (step(z, 1) * 2 + (1 - core), here)
    z_minus_other = (step(z, 3) * 2 + (1 - core), here)
    first = ((x_plus, x_minus), (y_plus, y_minus))
    second = ((y_plus, y_minus), (x_plus, x_minus))

    loads = []

    def load(src, dst):
        copy = pltpu.make_async_copy(src, dst, load_sem.at[len(loads)])
        copy.start()
        loads.append(copy)

    load(tok_ref, given.at[0])
    load(grad_ref, given.at[1])
    barrier = pltpu.get_barrier_semaphore()
    for device in (
        x_plus, x_minus, y_plus, y_minus, z_plus, z_minus, z_plus_other, z_minus_other, partner
    ):
        pl.semaphore_signal(barrier, inc=1, device_id=device, device_id_type=MESH)

    count = ROWS
    slot_row = lax.broadcasted_iota(jnp.int32, (2 * ROWS, count), 0)
    slot_node = ((z + (slot_row >> 3)) & 3) * 2 + ((core + (slot_row >> 2)) & 1)
    ids = id_ref[...].astype(F32)
    gates = gate_ref[...].astype(F32)
    id_rows = [ids[k : k + 1] for k in range(3)]
    gate_rows = [gates[k : k + 1] for k in range(3)]
    names = [
        [(id_rows[k] == (2 * slot_node + e).astype(F32)).astype(F32) for k in range(3)]
        for e in range(2)
    ]
    named = [names[e][0] + names[e][1] + names[e][2] for e in range(2)]
    member = jnp.maximum(named[0], named[1])
    earlier = (
        lax.broadcasted_iota(jnp.int32, (count, count), 0)
        < lax.broadcasted_iota(jnp.int32, (count, count), 1)
    ).astype(BF16)
    ranking = dot(member.astype(BF16), earlier, 1, 0)
    pick = jnp.where(ranking == (slot_row & 3).astype(F32), member, 0.0)
    pick_bf16 = pick.astype(BF16)
    side = [
        jnp.sum(pick * sum(names[e][k] * gate_rows[k] for k in range(3)), axis=1, keepdims=True)
        for e in range(2)
    ]
    side.append(jnp.sum(pick * named[0] * named[1], axis=1, keepdims=True))
    slot_lane = lax.broadcasted_iota(jnp.int32, (2 * ROWS, UNIT), 1)
    columns = sum(jnp.where(slot_lane == i, side[i], 0.0) for i in range(3)).astype(BF16)
    for s in range(8):
        outgo[s, :, width:wide] = columns[4 * s : 4 * s + 4]
    for copy in loads[:2]:
        copy.wait()
    stretch = width // 7

    def cut_rows(k, carry):
        at = pl.multiple_of(k * stretch, UNIT)
        for i, offset in enumerate((0, wide)):
            value = dot(pick_bf16, given[i, :, pl.ds(at, stretch)], 1, 0)
            for s in range(8):
                outgo[s, :, pl.ds(pl.multiple_of(at + offset, UNIT), stretch)] = value[
                    4 * s : 4 * s + 4
                ].astype(BF16)
        return carry

    lax.fori_loop(0, 7, cut_rows, 0)
    pl.semaphore_wait(barrier, 9)

    sends = []

    def send(src, dst, device):
        copy = pltpu.make_async_remote_copy(
            src_ref=src, dst_ref=dst, send_sem=send_sem.at[len(sends)],
            recv_sem=recv_sem.at[len(sends)], device_id=device, device_id_type=MESH,
        )
        copy.start()
        sends.append(copy)
        return copy

    across = {
        (0, 1): send(outgo.at[1], income.at[1], partner),
        (3, 0): send(outgo.at[6], income.at[2], z_minus),
        (1, 0): send(outgo.at[2], income.at[6], z_plus),
        (2, 0): send(outgo.at[4], relay.at[0], z_plus),
        (2, 1): send(outgo.at[5], relay.at[1], z_minus),
        (3, 1): send(outgo.at[7], income.at[3], z_minus_other),
        (1, 1): send(outgo.at[3], income.at[7], z_plus_other),
    }
    slots = ((0, 1, 2, 6), (4, 5, 3, 7))

    for i, ref in enumerate((wg_ref.at[0], wu_ref.at[0], sg_ref, su_ref)):
        load(ref, w_all.at[:, pl.ds(i * UNIT, UNIT)])
    for i, ref in enumerate((wd_ref.at[0], sd_ref)):
        load(ref, v_all.at[:, pl.ds(i * UNIT, UNIT)])

    def stack(h):
        def piece(at, size):
            return jnp.concatenate(
                [
                    (income if s else outgo)[s, :, pl.ds(at, size)].astype(F32)
                    for s in slots[h]
                ],
                0,
            ).astype(BF16)

        def one_stretch(k, carry):
            at = pl.multiple_of(k * stretch, UNIT)
            tt[h, 0, 0, :, pl.ds(at, stretch)] = piece(at, stretch)
            tg[h, 0, 0, :, pl.ds(at, stretch)] = piece(pl.multiple_of(at + wide, UNIT), stretch)
            return carry

        lax.fori_loop(0, 7, one_stretch, 0)
        tt[h, 0, 0, :, width:] = piece(width, UNIT)

    one, two, far = {}, {}, {}

    def first_hop(h):
        plus, minus = first[h]
        for part, (a, b) in enumerate(((tt, tg), (tg, tt))):
            one[h, "p", part] = send(a.at[h, 0, 0], a.at[h, 0, 3], plus)
            one[h, "m", part] = send(b.at[h, 0, 0], b.at[h, 0, 1], minus)

    for key in ((0, 1), (3, 0), (1, 0)):
        across[key].wait_recv()
    stack(0)
    first_hop(0)
    across[2, 0].wait_recv()
    forth = [send(relay.at[0], income.at[4], z_plus)]
    across[2, 1].wait_recv()
    forth.append(send(relay.at[1], income.at[5], z_minus_other))

    def second_hop(h, d):
        plus, minus = second[h]
        two[h, d, "pt"] = send(tt.at[h, 0, d], tt.at[h, 3, d], plus)
        two[h, d, "mg"] = send(tg.at[h, 0, d], tg.at[h, 1, d], minus)
        two[h, d, "pg"] = send(tg.at[h, 0, d], tg.at[h, 3, d], plus)
        two[h, d, "mt"] = send(tt.at[h, 0, d], tt.at[h, 1, d], minus)

    def pass_on(h):
        plus, minus = first[h]
        one[h, "p", 0].wait_recv()
        far[h, "p"] = send(tt.at[h, 0, 3], tt.at[h, 0, 2], plus)
        one[h, "m", 0].wait_recv()
        far[h, "m"] = send(tg.at[h, 0, 1], tg.at[h, 0, 2], minus)

    second_hop(0, 0)
    for copy in (across[3, 1], across[1, 1], *forth):
        copy.wait_recv()
    stack(1)
    first_hop(1)
    pass_on(0)
    second_hop(1, 0)
    pass_on(1)
    for h in range(2):
        one[h, "p", 1].wait_recv()
        second_hop(h, 3)
    for h in range(2):
        one[h, "m", 1].wait_recv()
        second_hop(h, 1)
    for h in range(2):
        far[h, "p"].wait_recv()
        far[h, "m"].wait_recv()
        second_hop(h, 2)

    rows = 2 * RING * ROWS
    expert = here // (RING * RING // 2)
    lane = lax.broadcasted_iota(jnp.int32, (RING * ROWS, UNIT), 1)
    depth = width // 7

    def compute(i):
        acc_p[...] = jnp.zeros_like(acc_p)
        acc_u[...] = jnp.zeros_like(acc_u)

        def forward(k, carry):
            at = pl.ds(pl.multiple_of(k * depth, UNIT), depth)
            t = jnp.concatenate([tt[h, i, :, :, at].reshape(rows // 2, depth) for h in range(2)], 0)
            g = jnp.concatenate([tg[h, i, :, :, at].reshape(rows // 2, depth) for h in range(2)], 0)
            acc_p[...] += dot(t, w_all[at, :], 1, 0)
            acc_u[...] += dot(g, v_all[at, :], 1, 0)
            return carry

        lax.fori_loop(0, 7, forward, 0)
        for h in range(2):
            mine = slice(h * rows // 2, (h + 1) * rows // 2)
            side = tt[h, i, :, :, width:].reshape(rows // 2, UNIT).astype(F32)
            gate = jnp.where(expert == 0, side[:, 0:1], side[:, 1:2])
            for j, weight in enumerate((gate, side[:, 2:3])):
                pre = acc_p[mine, 2 * j * UNIT : (2 * j + 1) * UNIT]
                up = acc_p[mine, (2 * j + 1) * UNIT : (2 * j + 2) * UNIT]
                upstream = acc_u[mine, j * UNIT : (j + 1) * UNIT]
                sig = 1.0 / (1.0 + jnp.exp(-pre))
                activ = pre * sig
                slope = sig * (1.0 + pre * (1.0 - sig))
                hidden = activ * up
                scaled = weight * upstream
                for place, value in (
                    (2 * j, scaled * up * slope),
                    (2 * j + 1, scaled * activ),
                    (4 + j, weight * hidden),
                ):
                    gg[h, i, :, :, place * UNIT : (place + 1) * UNIT] = value.astype(BF16).reshape(
                        RING, ROWS, UNIT
                    )
                if j == 0:
                    score = jnp.sum(hidden * upstream, axis=1, keepdims=True)
                    xx[h, i, :, :, width:] = (
                        jnp.where(lane == expert, score, 0.0).astype(BF16).reshape(RING, ROWS, UNIT)
                    )

        def backward(k, carry):
            at = pl.ds(pl.multiple_of(k * (depth // 2), UNIT), depth // 2)
            g = jnp.concatenate(
                [gg[h, i, :, :, : 4 * UNIT].reshape(rows // 2, 4 * UNIT) for h in range(2)], 0
            )
            value = dot(g, w_all[at, :], 1, 1).astype(BF16)
            for h in range(2):
                xx[h, i, :, :, at] = value[h * rows // 2 : (h + 1) * rows // 2].reshape(
                    RING, ROWS, depth // 2
                )
            return carry

        lax.fori_loop(0, 14, backward, 0)

    for copy in loads[2:]:
        copy.wait()
    compute(0)
    onward = {}
    for d in (0, 3, 1, 2):
        for h in range(2):
            plus, minus = second[h]
            two[h, d, "pt"].wait_recv()
            onward[h, d, "p"] = send(tt.at[h, 3, d], tt.at[h, 2, d], plus)
            two[h, d, "mg"].wait_recv()
            onward[h, d, "m"] = send(tg.at[h, 1, d], tg.at[h, 2, d], minus)
    for d in range(RING):
        for h in range(2):
            two[h, d, "pg"].wait_recv()
            two[h, d, "mt"].wait_recv()
    compute(1)
    compute(3)
    upper, lower = (2, 1), (3, 0)
    full = {}
    for h in range(2):
        plus, minus = second[h]
        for j in range(2):
            full[h, "p", lower[j]] = send(xx.at[h, 1, lower[j]], r2.at[h, 0, lower[j]], plus)
            full[h, "m", upper[j]] = send(xx.at[h, 3, upper[j]], r2.at[h, 1, upper[j]], minus)
    for copy in onward.values():
        copy.wait_recv()
    compute(2)
    back = {}
    for j in range(2):
        for h in range(2):
            plus, minus = second[h]
            back[h, "p", j] = send(xx.at[h, 2, upper[j]], r1.at[h, 0, j], plus)
            back[h, "m", j] = send(xx.at[h, 2, lower[j]], r1.at[h, 1, j], minus)

    everything = 2 * RING * RING * ROWS

    def weights(parity):
        def one_block(k, carry):
            b = 2 * k + parity
            at = pl.ds(pl.multiple_of(b * block, UNIT), block)
            t = tt[:, :, :, :, at].reshape(everything, block)
            g = tg[:, :, :, :, at].reshape(everything, block)
            a = dot(t, gg[:, :, :, :, : 4 * UNIT].reshape(everything, 4 * UNIT), 0, 0)
            c = dot(g, gg[:, :, :, :, 4 * UNIT :].reshape(everything, 2 * UNIT), 0, 0)
            dwg_ref[0, at] = a[:, :UNIT].astype(BF16)
            dwu_ref[0, at] = a[:, UNIT : 2 * UNIT].astype(BF16)
            dwd_ref[0, at] = c[:, :UNIT].astype(BF16)
            sw[parity, k, :, : 2 * UNIT] = a[:, 2 * UNIT :].astype(BF16)
            sw[parity, k, :, 2 * UNIT :] = c[:, UNIT:].astype(BF16)
            return carry

        lax.fori_loop(0, RING, one_block, 0)

    def add(dst, *srcs):
        total = dst[...].astype(F32)
        for src in srcs:
            total = total + src[...].astype(F32)
        dst[...] = total.astype(BF16)

    weights(1 - core)
    swap = send(sw.at[1 - core], pw, partner)
    for j in range(2):
        for h in range(2):
            plus, minus = second[h]
            back[h, "p", j].wait_recv()
            add(xx.at[h, 1, upper[j]], r1.at[h, 0, j])
            full[h, "p", upper[j]] = send(xx.at[h, 1, upper[j]], r2.at[h, 0, upper[j]], plus)
            back[h, "m", j].wait_recv()
            add(xx.at[h, 3, lower[j]], r1.at[h, 1, j])
            full[h, "m", lower[j]] = send(xx.at[h, 3, lower[j]], r2.at[h, 1, lower[j]], minus)
    weights(core)
    swap.wait_recv()

    def add_swap(k, carry):
        add(sw.at[core, k], pw.at[k])
        return carry

    lax.fori_loop(0, RING, add_swap, 0)
    low, high = pl.ds(0, half_block), pl.ds(half_block, half_block)
    z_back = (
        send(sw.at[core, step(z, 2), low], z1.at[0], z_plus),
        send(sw.at[core, step(z, 2), high], z1.at[1], z_minus),
    )
    z_full = [
        send(sw.at[core, step(z, 1), high], z2.at[0, high], z_plus),
        send(sw.at[core, step(z, 3), low], z2.at[1, low], z_minus),
    ]

    cut = (wide // UNIT + 1) // 2 * UNIT
    left, right = pl.ds(0, cut), pl.ds(cut, wide - cut)
    for d in (2, 3, 1, 0):
        for h in range(2):
            full[h, "p", d].wait_recv()
            full[h, "m", d].wait_recv()
            add(xx.at[h, 0, d], r2.at[h, 0, d], r2.at[h, 1, d])
            plus, minus = first[h]
            if d == 2:
                back[h, "P"] = send(xx.at[h, 0, 2, :, left], q1.at[h, 0, :, left], plus)
                back[h, "M"] = send(xx.at[h, 0, 2, :, right], q1.at[h, 1, :, right], minus)
            if d == 1:
                full[h, "P"] = send(xx.at[h, 0, 1, :, right], q2.at[h, 0, :, right], plus)
            if d == 3:
                full[h, "M"] = send(xx.at[h, 0, 3, :, left], q2.at[h, 1, :, left], minus)
    z_back[0].wait_recv()
    add(sw.at[core, step(z, 1), low], z1.at[0])
    z_full.append(send(sw.at[core, step(z, 1), low], z2.at[0, low], z_plus))
    z_back[1].wait_recv()
    add(sw.at[core, step(z, 3), high], z1.at[1])
    z_full.append(send(sw.at[core, step(z, 3), high], z2.at[1, high], z_minus))
    last = []
    for h in range(2):
        plus, minus = first[h]
        back[h, "P"].wait_recv()
        add(xx.at[h, 0, 1, :, left], q1.at[h, 0, :, left])
        last.append(send(xx.at[h, 0, 1, :, left], q2.at[h, 0, :, left], plus))
        back[h, "M"].wait_recv()
        add(xx.at[h, 0, 3, :, right], q1.at[h, 1, :, right])
        last.append(send(xx.at[h, 0, 3, :, right], q2.at[h, 1, :, right], minus))
    for h in range(2):
        full[h, "P"].wait_recv()
        full[h, "M"].wait_recv()
        last[2 * h].wait_recv()
        last[2 * h + 1].wait_recv()

        def one_stretch(k, carry, h=h):
            at = pl.ds(pl.multiple_of(k * 3 * UNIT, UNIT), 3 * UNIT)
            total = xx[h, 0, 0, :, at].astype(F32)
            for i in range(2):
                total = total + q2[h, i, :, at].astype(F32)
            for s in range(4):
                answer[slots[h][s], :, at] = total[4 * s : 4 * s + 4].astype(BF16)
            return carry

        lax.fori_loop(0, wide // (3 * UNIT), one_stretch, 0)
        if h == 0:
            home = [
                send(answer.at[2], reply.at[6], z_plus),
                send(answer.at[6], reply.at[2], z_minus),
                send(answer.at[1], reply.at[1], partner),
            ]
        else:
            home += [
                send(answer.at[4], relay_back.at[0], z_plus),
                send(answer.at[5], relay_back.at[1], z_minus),
                send(answer.at[3], reply.at[7], z_plus_other),
                send(answer.at[7], reply.at[3], z_minus_other),
            ]
    for copy in z_full:
        copy.wait_recv()
    total = sw[core, z].astype(F32) + z2[0].astype(F32) + z2[1].astype(F32)
    for j, ref in enumerate((dsg_ref, dsu_ref, dsd_ref)):
        ref[...] = total[:, j * UNIT : (j + 1) * UNIT].astype(BF16)
    home[3].wait_recv()
    home.append(send(relay_back.at[0], reply.at[4], z_plus))
    home[4].wait_recv()
    home.append(send(relay_back.at[1], reply.at[5], z_minus_other))
    for i in (0, 1, 2, 5, 6, 7, 8):
        home[i].wait_recv()

    def answers(at, size):
        return jnp.concatenate(
            [(answer if s == 0 else reply)[s, :, pl.ds(at, size)].astype(F32) for s in range(8)], 0
        )

    def finish(k, carry):
        at = pl.multiple_of(k * stretch, UNIT)
        total = dot(pick_bf16, answers(at, stretch).astype(BF16), 0, 0)
        dx_ref[:, pl.ds(at, stretch)] = total.astype(BF16)
        return carry

    lax.fori_loop(0, 7, finish, 0)
    score = answers(width, UNIT)
    for k in range(3):
        dgate_ref[k : k + 1] = jnp.sum(
            pick * (names[0][k] * score[:, 0:1] + names[1][k] * score[:, 1:2]),
            axis=0, keepdims=True,
        )
    for copy in sends:
        copy.wait_send()


def hand_on(*refs):
    ins, outs, sems = refs[:8], refs[8:16], refs[16]
    copies = [pltpu.make_async_copy(*pair, sems.at[i]) for i, pair in enumerate(zip(ins, outs))]
    for copy in copies:
        copy.start()
    for copy in copies:
        copy.wait()


SENDS = 103 + 9 + 9


def expert_layer(tokens, grad_out, gates, ids, w_gate, w_up, w_down, s_gate, s_up, s_down):
    width = s_gate.shape[0]
    wide = width + UNIT
    block = width // 8
    shape = jax.ShapeDtypeStruct
    anywhere = pl.BlockSpec(memory_space=pl.ANY)
    inside = pl.BlockSpec(memory_space=pltpu.VMEM)
    dx, dgates, *grads = pl.pallas_call(
        body,
        out_shape=(
            pltpu.VMEM(tokens.shape, BF16),
            pltpu.VMEM(gates.shape[::-1], F32),
            *(pltpu.VMEM(w_gate.shape, BF16) for _ in range(3)),
            *(pltpu.VMEM((block, UNIT), BF16) for _ in range(3)),
        ),
        in_specs=[anywhere] * 2 + [inside] * 2 + [anywhere] * 6,
        out_specs=(inside,) * 8,
        scratch_shapes=[
            pltpu.VMEM((2, ROWS, width), BF16),
            pltpu.VMEM((8, 4, wide + width), BF16),
            pltpu.VMEM((8, 4, wide + width), BF16),
            pltpu.VMEM((2, 4, wide + width), BF16),
            pltpu.VMEM((8, 4, wide), BF16),
            pltpu.VMEM((8, 4, wide), BF16),
            pltpu.VMEM((2, 4, wide), BF16),
            pltpu.VMEM((2, RING, RING, ROWS, wide), BF16),
            pltpu.VMEM((2, RING, RING, ROWS, width), BF16),
            pltpu.VMEM((2, RING, RING, ROWS, wide), BF16),
            pltpu.VMEM((width, 4 * UNIT), BF16),
            pltpu.VMEM((width, 2 * UNIT), BF16),
            pltpu.VMEM((2, RING, RING, ROWS, 6 * UNIT), BF16),
            pltpu.VMEM((2 * RING * ROWS, 4 * UNIT), F32),
            pltpu.VMEM((2 * RING * ROWS, 2 * UNIT), F32),
            pltpu.VMEM((2, 2, 2, ROWS, wide), BF16),
            pltpu.VMEM((2, 2, RING, ROWS, wide), BF16),
            pltpu.VMEM((2, 2, ROWS, wide), BF16),
            pltpu.VMEM((2, 2, ROWS, wide), BF16),
            pltpu.VMEM((2, RING, block, 3 * UNIT), BF16),
            pltpu.VMEM((RING, block, 3 * UNIT), BF16),
            pltpu.VMEM((2, block // 2, 3 * UNIT), BF16),
            pltpu.VMEM((2, block, 3 * UNIT), BF16),
            pltpu.SemaphoreType.DMA((SENDS,)),
            pltpu.SemaphoreType.DMA((SENDS,)),
            pltpu.SemaphoreType.DMA((8,)),
        ],
        compiler_params=pltpu.CompilerParams(
            collective_id=0, has_side_effects=True, vmem_limit_bytes=60500000
        ),
    )(tokens, grad_out, gates.T, ids.T, w_gate, w_up, w_down, s_gate, s_up, s_down)
    outs = (dx, *grads, dgates)
    dx, *grads, dgates = pl.pallas_call(
        hand_on,
        out_shape=tuple(shape(o.shape, o.dtype) for o in outs),
        in_specs=[inside] * 8,
        out_specs=(anywhere,) * 8,
        scratch_shapes=[pltpu.SemaphoreType.DMA((8,))],
        compiler_params=pltpu.CompilerParams(vmem_limit_bytes=8 * 2**20),
    )(*outs)
    return (dx, dgates.T, *grads)


def solution(mesh):
    flat = P(("node", "local"), None)
    routed = P("node", None, "local")
    shared = P(None, "local")
    return jax.shard_map(
        expert_layer,
        mesh=mesh,
        in_specs=(flat,) * 4 + (routed,) * 3 + (shared,) * 3,
        out_specs=(flat, flat) + (routed,) * 3 + (P("node", "local"),) * 3,
        check_vma=False,
    )
```
